128 devices in a mesh: row: 8 (over x, z_hi), col: 16 (over z_lo, y, core).
Axes of the slice: x: 4, y: 4, z: 4 (z_hi: 2, z_lo: 2; z = z_hi * 2 + z_lo), core: 2. Of those that a mesh axis runs over, the one named last changes fastest.
Arguments:
- covariance: float32 [16384, 16384], P('row', 'col'), may hold values from -1 to 560
- seed_index: int32 [128], replicated, may hold values from 0 to 16383, as said below
Outputs:
- basis: float32 [16384, 384], P('row')
- projection: float32 [384, 256], replicated
- first_pass: float32 [384, 256], replicated
The draws below stay inside these ranges and needn't reach their ends.
Inputs may be any that keep to these rules, and one draw needn't show every extreme that they name: `seed_index`: 128 distinct column indices.
All inputs are finite; a program needn't handle non-finite values.
Results may differ from the reference program's by a relative error of at most 0.00019.
Values sent between devices are 32-bit elements; how exact they have to be, the bound alone decides.
A program may use at most 128 MiB of HBM per device.

```python
import jax
import jax.numpy as jnp
from jax import lax

N = 16384
B = 128
ITERS = 2


def draw_covariance(key, part):
    first_key = jax.random.fold_in(key, 11)
    second_key = jax.random.fold_in(key, 12)
    place = jnp.arange(N, dtype=jnp.float32) / jnp.float32(N - 1)
    noise = jax.random.normal(first_key, (N, N), jnp.float32)
    loading = jnp.exp(jax.random.uniform(second_key, (N,), jnp.float32, jnp.log(8.0), jnp.log(40.0)))
    loading = loading * (1.0 + 2.0 * place)
    symmetric = (noise + noise.T) * (3.0 / (2.0 * N) ** 0.5)
    return symmetric + jnp.diag(loading)


def draw_seed_index(key, part):
    order = jax.random.permutation(jax.random.fold_in(key, 21), N)
    return order[:B].astype(jnp.int32)


def setup_inputs(seed: int = 0) -> dict:
    arg_keys = jax.random.split(jax.random.key(seed), 3)
    covariance = draw_covariance(jax.random.fold_in(arg_keys[2], 71), 0)
    seed_index = draw_seed_index(jax.random.fold_in(arg_keys[2], 71), 0)
    return dict(covariance=covariance, seed_index=seed_index)


def product(left, right):
    return jnp.dot(left.astype(jnp.float32), right.astype(jnp.float32), precision=lax.Precision.HIGHEST, preferred_element_type=jnp.float32)

def orthonormal(block):
    gram = product(block.T, block)
    lower = jnp.linalg.cholesky(gram)
    basis_block = jax.scipy.linalg.solve_triangular(lower, block.T, lower=True).T
    return (basis_block, lower.T)

def reference(covariance, seed_index):
    start = jnp.take(covariance, seed_index.astype(jnp.int32), axis=1)
    current, upper = orthonormal(start)
    blocks = [current]
    projection = jnp.zeros(((ITERS + 1) * B, ITERS * B), jnp.float32)
    first_pass = jnp.zeros(((ITERS + 1) * B, ITERS * B), jnp.float32)
    for section in range(ITERS):
        image = product(covariance, current)
        stacked = jnp.concatenate(blocks, axis=1)
        first = product(stacked.T, image)
        once = image - product(stacked, first)
        second = product(stacked.T, once)
        twice = once - product(stacked, second)
        current, upper = orthonormal(twice)
        projection = projection.at[:(section + 1) * B, section * B:(section + 1) * B].set(first + second)
        projection = projection.at[(section + 1) * B:(section + 2) * B, section * B:(section + 1) * B].set(upper)
        first_pass = first_pass.at[:(section + 1) * B, section * B:(section + 1) * B].set(first)
        blocks.append(current)
    basis = jnp.concatenate(blocks, axis=1) * jnp.float32(N ** 0.5)
    return (basis, projection, first_pass)
```

```python
import jax
import jax.numpy as jnp
from jax import lax
from jax.experimental import pallas as pl
from jax.experimental.pallas import tpu as pltpu
from jax.sharding import PartitionSpec as P

N = 16384
B = 128
ITERS = 2
ROWS = 2048
COLS = 1024
NB = 16
MESH = pl.DeviceIdType.MESH
F32 = jnp.float32
BF16 = jnp.bfloat16
NN = (((1,), (0,)), ((), ()))
NT = (((1,), (1,)), ((), ()))
TN = (((0,), (0,)), ((), ()))


def exact(a, b, dims=NN):
    return lax.dot_general(a, b, dims, precision=lax.Precision.HIGHEST, preferred_element_type=F32)


def halves(a):
    high = a.astype(BF16)
    return high, (a - high.astype(F32)).astype(BF16)


def fine(a, b, dims=NN):
    ah, al = halves(a)
    bh, bl = halves(b)

    def dot(x, y):
        return lax.dot_general(x, y, dims, preferred_element_type=F32)

    return dot(ah, bh) + (dot(ah, bl) + dot(al, bh))


def factor(gram, aug, low):
    rows = lax.broadcasted_iota(jnp.int32, (B, B), 0)
    lanes = lax.broadcasted_iota(jnp.int32, (B, B), 1)
    aug[:, :B] = gram
    aug[:, B:] = jnp.where(rows == lanes, 1.0, 0.0).astype(F32)
    lane = lax.broadcasted_iota(jnp.int32, (NB, B), 1)
    sub = lax.broadcasted_iota(jnp.int32, (NB, B), 0)

    def panel(p, carry):
        o = pl.multiple_of(p * NB, NB)
        left = aug[pl.ds(o, NB), :B]
        right = aug[pl.ds(o, NB), B:]
        cols = []
        for t in range(NB):
            one = jnp.sum(jnp.where(lane == o + t, left, 0.0), axis=1, keepdims=True)
            cols.append(jnp.broadcast_to(one, (NB, B)))
        for t in range(NB):
            inv = lax.rsqrt(cols[t][t : t + 1, :])
            scale = jnp.where(sub == t, inv, 1.0)
            ratio = jnp.where(sub > t, cols[t] * inv, 0.0)
            left = left * scale
            right = right * scale
            left = left - ratio * left[t : t + 1, :]
            right = right - ratio * right[t : t + 1, :]
            for u in range(t + 1, NB):
                cols[u] = cols[u] - ratio * (cols[u][t : t + 1, :] * inv)
        left = jnp.where(lane >= o, left, 0.0)
        low[pl.ds(o, NB), :B] = jnp.where(lane >= o + sub, left, 0.0)
        low[pl.ds(o, NB), B:] = right
        both = jnp.concatenate([left, right], axis=1)
        aug[...] = aug[...] - exact(left, both, TN)
        return carry

    lax.fori_loop(0, B // NB, panel, 0)


def kernel(
    seed, cov, basis, projection, first_pass,
    cvm, chi, clo, stp, rs1, shard, vcol, srow, ypart, d2d, yown, rs2, yrow, q0, w1, wt, y1p, rs3, zrow, q1,
    scat, aug, low0, low1, low2, part, ga, gb, ha, hb, ia, ib, ja, jb, ka, kb,
    csem, rs1_s, rs1_r, ag1_s, ag1_r, tg1_s, tg1_r, d2d_s, d2d_r, rs2_s, rs2_r, ag2_s, ag2_r, fw_s, rs3_s, rs3_r, tg2_s, tg2_r,
    sa_s, sa_r, sb_s, sb_r,
):
    r = lax.axis_index("row")
    c = lax.axis_index("col")
    core = lax.rem(c, 2)
    chip = lax.div(c, 2)
    partner = c + 1 - 2 * core

    def loop(lo, hi, body):
        def run(i, carry):
            body(i)
            return carry

        lax.fori_loop(lo, hi, run, 0)

    def remote(src, dst, ssem, rsem, dev):
        return pltpu.make_async_remote_copy(src, dst, ssem, rsem, device_id=dev, device_id_type=MESH)

    def row_peer(k):
        return lax.rem(r + k, 8)

    def load(i):
        return pltpu.make_async_copy(cov.at[pl.ds(i * 256, 256)], cvm.at[pl.ds(i * 256, 256)], csem.at[i])

    loop(0, 8, lambda i: load(i).start())
    loop(0, 8, lambda i: load(i).wait())

    def gather(i):
        lines = []
        for t in range(8):
            at = seed[i * 8 + t] - r * ROWS
            inside = (at >= 0) & (at < ROWS)
            line = cvm[pl.ds(jnp.clip(at, 0, ROWS - 1), 1), :]
            lines.append(jnp.where(inside, line, 0.0))
        block = jnp.concatenate(lines, axis=0)
        for b in range(8):
            stp[b, pl.ds(pl.multiple_of(i * 8, 8), 8), :] = block[:, b * B : (b + 1) * B]

    loop(0, B // 8, gather)

    def row_scatter(src, dst, ssem, rsem):
        def send(k):
            to = row_peer(k)
            remote(src.at[to], dst.at[r], ssem.at[k], rsem.at[r], (to, c)).start()

        loop(1, 8, send)

    def row_scatter_sum(src, dst, ssem, rsem):
        def wait(k):
            src_row = row_peer(k)
            remote(src.at[0], dst.at[src_row], ssem.at[k], rsem.at[src_row], (r, c)).wait_recv()

        loop(1, 8, wait)
        dst[r] = src[r]
        total = dst[0]
        for i in range(1, 8):
            total = total + dst[i]
        return total

    row_scatter(stp, rs1, rs1_s, rs1_r)

    def split(i):
        blk = cvm[pl.ds(pl.multiple_of(i * B, B), B), :]
        high, rest = halves(blk)
        chi[lax.div(i, 2), lax.rem(i, 2)] = high
        clo[lax.div(i, 2), lax.rem(i, 2)] = rest

    loop(0, 16, split)

    start = row_scatter_sum(stp, rs1, rs1_s, rs1_r).T
    shard[0] = start
    vcol[r] = start

    def ag1(k):
        return remote(shard.at[0], vcol.at[r], ag1_s.at[k], ag1_r.at[r], (row_peer(k), c))

    loop(1, 8, lambda k: ag1(k).start())

    slot = core * 8 + r

    def place(src, dst, ssem, rsem):
        def send(k):
            to = lax.rem(c + k, 16)

            @pl.when(jnp.logical_or(chip != r, to != c))
            def _():
                remote(src, dst.at[slot], ssem.at[k], rsem.at[slot], (chip, to)).start()

        loop(0, 16, send)

    def placed(src, dst, ssem, rsem):
        def wait(s):
            mine = jnp.logical_and(lax.rem(s, 8) == r, 2 * r + lax.div(s, 8) == c)

            @pl.when(jnp.logical_not(mine))
            def _():
                remote(src, dst.at[s], ssem.at[0], rsem.at[s], (r, c)).wait_recv()

        loop(0, 16, wait)

        @pl.when(chip == r)
        def _():
            dst[slot] = src[...]

    def place_sent(src, dst, ssem, rsem):
        def wait(k):
            to = lax.rem(c + k, 16)

            @pl.when(jnp.logical_or(chip != r, to != c))
            def _():
                remote(src, dst.at[slot], ssem.at[k], rsem.at[slot], (chip, to)).wait_send()

        loop(0, 16, wait)

    place(shard.at[0], srow, tg1_s, tg1_r)

    def ag1_wait(k):
        src_row = row_peer(k)
        remote(shard.at[0], vcol.at[src_row], ag1_s.at[k], ag1_r.at[src_row], (r, c)).wait_recv()

    loop(1, 8, ag1_wait)

    def cat(i):
        high, rest = halves(vcol[i])
        scat[pl.ds(pl.multiple_of(i * B, B), B), :B] = high
        scat[pl.ds(pl.multiple_of(i * B, B), B), B:] = rest

    loop(0, 8, cat)

    def times(first, parity):
        a = chi[pl.ds(first, 4), parity].reshape(512, COLS)
        b = clo[pl.ds(first, 4), parity].reshape(512, COLS)
        full = jnp.dot(a, scat[...], preferred_element_type=F32) + jnp.dot(b, scat[...], preferred_element_type=F32)
        return (full[:, :B] + full[:, B:]).reshape(4, B, B)

    def across(h):
        return remote(ypart.at[pl.ds(h * 4, 4)], d2d.at[pl.ds(h * 4, 4)], d2d_s.at[h], d2d_r.at[h], (r, partner))

    def theirs(h):
        ypart[pl.ds(h * 4, 4)] = times(h * 4, 1 - core)
        across(h).start()

    loop(0, 2, theirs)

    def ours(h):
        yown[pl.ds(h * 4, 4)] = times(h * 4, core)

    loop(0, 2, ours)

    def rs2_send(i):
        return remote(yown.at[i], rs2.at[chip], rs2_s.at[i], rs2_r.at[chip], (r, 2 * i + core))

    def combine(h):
        across(h).wait_recv()
        for t in range(4):
            i = h * 4 + t
            yown[i] = yown[i] + d2d[i]

            @pl.when(i != chip)
            def _():
                rs2_send(i).start()

    loop(0, 2, combine)

    def small_start(src, buf, n, tag):
        buf[r] = src[pl.ds(pl.multiple_of(c * n, n), n), :]

        def send(k):
            remote(buf.at[r], buf.at[r], sa_s.at[tag, k], sa_r.at[tag, r], (row_peer(k), c)).start()

        loop(1, 8, send)

    def small_middle(buf, out, n, tag):
        def wait(k):
            src_row = row_peer(k)
            remote(buf.at[r], buf.at[src_row], sa_s.at[tag, k], sa_r.at[tag, src_row], (r, c)).wait_recv()

        loop(1, 8, wait)
        total = buf[0]
        for i in range(1, 8):
            total = total + buf[i]
        out[c] = total

        def send(k):
            to = lax.rem(c + k, 16)
            remote(out.at[c], out.at[c], sb_s.at[tag, k], sb_r.at[tag, c], (r, to)).start()

        loop(1, 16, send)

    def small_end(out, n, tag):
        def wait(k):
            src_col = lax.rem(c + k, 16)
            remote(out.at[c], out.at[src_col], sb_s.at[tag, k], sb_r.at[tag, src_col], (r, c)).wait_recv()

        loop(1, 16, wait)
        return out[...].reshape(16 * n, B)

    def small_sent(buf, out, tag):
        loop(1, 8, lambda k: remote(buf.at[r], buf.at[r], sa_s.at[tag, k], sa_r.at[tag, r], (r, c)).wait_send())
        loop(1, 16, lambda k: remote(out.at[c], out.at[c], sb_s.at[tag, k], sb_r.at[tag, c], (r, c)).wait_send())

    placed(shard.at[0], srow, tg1_s, tg1_r)
    part[0:B, :] = jnp.zeros((B, B), F32)

    def gram0(i):
        blk = srow[pl.ds(2 * i, 2)].reshape(256, B)
        part[0:B, :] += fine(blk, blk, TN)

    loop(0, 8, gram0)
    small_start(part, ga, 8, 0)

    def rs2_wait(i):
        @pl.when(i != chip)
        def _():
            remote(yown.at[i], rs2.at[i], rs2_s.at[i], rs2_r.at[i], (r, c)).wait_recv()

    loop(0, 8, rs2_wait)
    rs2[chip] = yown[chip]
    total = rs2[0]
    for i in range(1, 8):
        total = total + rs2[i]
    yrow[c] = total

    def ag2(i):
        return remote(yrow.at[c], yrow.at[c], ag2_s.at[i], ag2_r.at[c], (r, 2 * i + core))

    def ag2_send(i):
        @pl.when(i != chip)
        def _():
            ag2(i).start()

    loop(0, 8, ag2_send)
    to_partner = remote(yrow.at[c], yrow.at[c], fw_s.at[chip], ag2_r.at[c], (r, partner))
    to_partner.start()
    small_middle(ga, gb, 8, 0)

    def forward(i):
        return remote(yrow.at[2 * i + core], yrow.at[2 * i + core], fw_s.at[i], ag2_r.at[2 * i + core], (r, partner))

    def relay(k):
        i = lax.rem(chip + k, 8)
        remote(yrow.at[c], yrow.at[2 * i + core], ag2_s.at[i], ag2_r.at[2 * i + core], (r, c)).wait_recv()
        forward(i).start()

    loop(1, 8, relay)
    gram = small_end(gb, 8, 0)
    factor(gram, aug, low0)
    inv0 = low0[:, B:]

    def first_q(i):
        v = fine(srow[i], inv0, NT)
        q0[i] = v
        basis[pl.ds(pl.multiple_of(i * B, B), B), 0:B] = v * F32(N**0.5)

    loop(0, 16, first_q)

    def relayed(i):
        s = 2 * i + 1 - core
        remote(yrow.at[c], yrow.at[s], fw_s.at[i], ag2_r.at[s], (r, c)).wait_recv()

    loop(0, 8, relayed)

    part[0:B, :] = jnp.zeros((B, B), F32)

    def first_h(i):
        v = fine(yrow[i], inv0, NT)
        zrow[i] = v
        part[0:B, :] += fine(q0[i], v, TN)

    loop(0, 16, first_h)
    small_start(part, ha, 8, 1)
    small_middle(ha, hb, 8, 1)
    h1 = small_end(hb, 8, 1)
    first_pass[...] = jnp.zeros((3 * B, 2 * B), F32)
    projection[...] = jnp.zeros((3 * B, 2 * B), F32)
    first_pass[0:B, 0:B] = h1

    part[0 : 2 * B, :] = jnp.zeros((2 * B, B), F32)

    def once(i):
        w = zrow[i] - fine(q0[i], h1)
        w1[i] = w
        high, rest = halves(w.T)
        o = pl.multiple_of(i * B, B)
        wt[0:B, pl.ds(o, B)] = high
        wt[B : 2 * B, pl.ds(o, B)] = rest

    loop(0, 16, once)

    def times_t(k):
        q = lax.rem(lax.div(r, 2) + 1 + k, 4)
        o = pl.multiple_of(q * 256, 256)
        a = chi[:, :, :, pl.ds(o, 256)].reshape(ROWS, 256)
        b = clo[:, :, :, pl.ds(o, 256)].reshape(ROWS, 256)
        full = jnp.dot(wt[...], a, preferred_element_type=F32) + jnp.dot(wt[...], b, preferred_element_type=F32)
        half = full[:B, :] + full[B:, :]
        y1p[2 * q] = half[:, :B]
        y1p[2 * q + 1] = half[:, B:]
        for t in range(2):
            to = 2 * q + t

            @pl.when(to != r)
            def _():
                remote(y1p.at[to], rs3.at[r], rs3_s.at[to], rs3_r.at[r], (to, c)).start()

    loop(0, 4, times_t)

    def second_part(i):
        w = w1[i]
        part[0:B, :] += fine(q0[i], w, TN)
        part[B : 2 * B, :] += fine(w, w, TN)

    loop(0, 16, second_part)
    small_start(part, ia, 16, 2)

    def rs3_wait(i):
        @pl.when(i != r)
        def _():
            remote(y1p.at[i], rs3.at[i], rs3_s.at[i], rs3_r.at[i], (r, c)).wait_recv()

    loop(0, 8, rs3_wait)
    rs3[r] = y1p[r]
    total = rs3[0]
    for i in range(1, 8):
        total = total + rs3[i]
    shard[1] = total.T
    place(shard.at[1], q1, tg2_s, tg2_r)

    small_middle(ia, ib, 16, 2)
    sums = small_end(ib, 16, 2)
    h2 = sums[0:B, :]
    projection[0:B, 0:B] = h1 + h2
    factor(sums[B : 2 * B, :] - exact(h2, h2, TN), aug, low1)
    projection[B : 2 * B, 0:B] = low1[:, :B]
    inv1 = low1[:, B:]

    def second_q(i):
        v = fine(w1[i] - fine(q0[i], h2), inv1, NT)
        w1[i] = v
        basis[pl.ds(pl.multiple_of(i * B, B), B), B : 2 * B] = v * F32(N**0.5)

    loop(0, 16, second_q)
    placed(shard.at[1], q1, tg2_s, tg2_r)

    part[0 : 2 * B, :] = jnp.zeros((2 * B, B), F32)

    def image1(i):
        v = fine(q1[i] - fine(zrow[i], h2), inv1, NT)
        zrow[i] = v
        part[0:B, :] += fine(q0[i], v, TN)
        part[B : 2 * B, :] += fine(w1[i], v, TN)

    loop(0, 16, image1)
    small_start(part, ja, 16, 3)
    small_middle(ja, jb, 16, 3)
    h1b = small_end(jb, 16, 3)
    first_pass[0 : 2 * B, B : 2 * B] = h1b
    part[...] = jnp.zeros((3 * B, B), F32)

    def once1(i):
        w = zrow[i] - (fine(q0[i], h1b[0:B]) + fine(w1[i], h1b[B : 2 * B]))
        zrow[i] = w
        part[0:B, :] += fine(q0[i], w, TN)
        part[B : 2 * B, :] += fine(w1[i], w, TN)
        part[2 * B : 3 * B, :] += fine(w, w, TN)

    loop(0, 16, once1)
    small_start(part, ka, 24, 4)
    small_middle(ka, kb, 24, 4)
    sums1 = small_end(kb, 24, 4)
    h2b = sums1[0 : 2 * B, :]
    projection[0 : 2 * B, B : 2 * B] = h1b + h2b
    factor(sums1[2 * B : 3 * B, :] - exact(h2b, h2b, TN), aug, low2)
    projection[2 * B : 3 * B, B : 2 * B] = low2[:, :B]
    inv2 = low2[:, B:]

    def third_q(i):
        w = zrow[i] - (fine(q0[i], h2b[0:B]) + fine(w1[i], h2b[B : 2 * B]))
        basis[pl.ds(pl.multiple_of(i * B, B), B), 2 * B : 3 * B] = fine(w, inv2, NT) * F32(N**0.5)

    loop(0, 16, third_q)

    loop(1, 8, lambda k: remote(stp.at[0], rs1.at[r], rs1_s.at[k], rs1_r.at[r], (r, c)).wait_send())
    loop(1, 8, lambda k: ag1(k).wait_send())
    place_sent(shard.at[0], srow, tg1_s, tg1_r)
    loop(0, 2, lambda h: across(h).wait_send())

    def sent(i):
        @pl.when(i != chip)
        def _():
            rs2_send(i).wait_send()
            ag2(i).wait_send()

        forward(i).wait_send()

        @pl.when(i != r)
        def _():
            remote(y1p.at[i], rs3.at[r], rs3_s.at[i], rs3_r.at[r], (r, c)).wait_send()

    loop(0, 8, sent)
    place_sent(shard.at[1], q1, tg2_s, tg2_r)
    for tag, (a, b) in enumerate(((ga, gb), (ha, hb), (ia, ib), (ja, jb), (ka, kb))):
        small_sent(a, b, tag)


def local(covariance, seed_index):
    v = pltpu.VMEM
    dma = pltpu.SemaphoreType.DMA
    blocks8 = v((8, B, B), F32)
    blocks16 = v((16, B, B), F32)
    small = []
    for n in (8, 8, 16, 16, 24):
        small += [v((8, n, B), F32), v((16, n, B), F32)]
    scratch = [
        v((ROWS, COLS), F32), v((8, 2, B, COLS), BF16), v((8, 2, B, COLS), BF16),
        blocks8, blocks8, v((2, B, B), F32), blocks8, blocks16,
        blocks8, blocks8, blocks8, blocks8, blocks16,
        blocks16, blocks16, v((2 * B, ROWS), BF16), blocks8, blocks8, blocks16, blocks16,
        v((COLS, 2 * B), BF16), v((B, 2 * B), F32), v((B, 2 * B), F32), v((B, 2 * B), F32), v((B, 2 * B), F32),
        v((3 * B, B), F32), *small,
        dma((8,)), dma((8,)), dma((8,)), dma((8,)), dma((8,)), dma((16,)), dma((16,)),
        dma((2,)), dma((2,)), dma((8,)), dma((8,)), dma((8,)), dma((16,)), dma((8,)), dma((8,)), dma((8,)),
        dma((16,)), dma((16,)),
        dma((5, 8)), dma((5, 8)), dma((5, 16)), dma((5, 16)),
    ]
    basis, projection, first_pass = pl.pallas_call(
        kernel,
        out_shape=(
            jax.ShapeDtypeStruct((ROWS, 3 * B), F32),
            jax.ShapeDtypeStruct((3 * B, 2 * B), F32),
            jax.ShapeDtypeStruct((3 * B, 2 * B), F32),
        ),
        in_specs=[pl.BlockSpec(memory_space=pltpu.SMEM), pl.BlockSpec(memory_space=pl.ANY)],
        out_specs=[pl.BlockSpec(memory_space=pltpu.VMEM)] * 3,
        scratch_shapes=scratch,
        compiler_params=pltpu.CompilerParams(has_side_effects=True, vmem_limit_bytes=60 * 2**20),
        name="lanczos",
    )(seed_index, covariance)
    return basis, projection, first_pass


def solution(mesh):
    return jax.shard_map(
        local,
        mesh=mesh,
        in_specs=(P("row", "col"), P()),
        out_specs=(P("row", None), P(), P()),
        check_vma=False,
    )
```

```python
import jax
import jax.numpy as jnp
from jax import lax
from jax.experimental import pallas as pl
from jax.experimental.pallas import tpu as pltpu
from jax.sharding import PartitionSpec as P

N = 16384
B = 128
ITERS = 2
ROWS = 2048
COLS = 1024
NB = 16
MESH = pl.DeviceIdType.MESH
F32 = jnp.float32
BF16 = jnp.bfloat16
NN = (((1,), (0,)), ((), ()))
NT = (((1,), (1,)), ((), ()))
TN = (((0,), (0,)), ((), ()))


def exact(a, b, dims=NN):
    return lax.dot_general(a, b, dims, precision=lax.Precision.HIGHEST, preferred_element_type=F32)


def halves(a):
    high = a.astype(BF16)
    return high, (a - high.astype(F32)).astype(BF16)


def fine(a, b, dims=NN):
    ah, al = halves(a)
    bh, bl = halves(b)

    def dot(x, y):
        return lax.dot_general(x, y, dims, preferred_element_type=F32)

    both = dot(jnp.concatenate([ah, al], axis=0), bh)
    n = a.shape[0]
    return both[:n] + (both[n:] + dot(ah, bl))


def factor(gram, aug, low):
    rows = lax.broadcasted_iota(jnp.int32, (B, B), 0)
    lanes = lax.broadcasted_iota(jnp.int32, (B, B), 1)
    aug[:, :B] = gram
    aug[:, B:] = jnp.where(rows == lanes, 1.0, 0.0).astype(F32)
    lane = lax.broadcasted_iota(jnp.int32, (NB, B), 1)
    sub = lax.broadcasted_iota(jnp.int32, (NB, B), 0)

    def panel(p, carry):
        o = pl.multiple_of(p * NB, NB)
        left = aug[pl.ds(o, NB), :B]
        right = aug[pl.ds(o, NB), B:]
        cols = []
        for t in range(NB):
            one = jnp.sum(jnp.where(lane == o + t, left, 0.0), axis=1, keepdims=True)
            cols.append(jnp.broadcast_to(one, (NB, B)))
        for t in range(NB):
            inv = lax.rsqrt(cols[t][t : t + 1, :])
            scale = jnp.where(sub == t, inv, 1.0)
            ratio = jnp.where(sub > t, cols[t] * inv, 0.0)
            left = left * scale
            right = right * scale
            left = left - ratio * left[t : t + 1, :]
            right = right - ratio * right[t : t + 1, :]
            for u in range(t + 1, NB):
                cols[u] = cols[u] - ratio * (cols[u][t : t + 1, :] * inv)
        left = jnp.where(lane >= o, left, 0.0)
        low[pl.ds(o, NB), :B] = jnp.where(lane >= o + sub, left, 0.0)
        low[pl.ds(o, NB), B:] = right
        both = jnp.concatenate([left, right], axis=1)
        aug[...] = aug[...] - exact(left, both, TN)
        return carry

    lax.fori_loop(0, B // NB, panel, 0)


def kernel(
    seed, cov, p_out, l_out, h_out, f_out,
    cvm, chi, clo, stp, rs1, vcol, st, ypart, d2d, yown, rs2, yt, zt, pt, wt, y1p, rs3, tsh, last, projection, first_pass,
    scat, aug, low0, low1, low2, ga, gb, ha, hb, ia, ib, ja, jb, ka, kb,
    csem, osem, rs1_s, rs1_r, ag1_s, ag1_r, t_s, t_r, d2d_s, d2d_r, rs2_s, rs2_r, ag_s, ag_r, fw_s, rs3_s, rs3_r,
    sa_s, sa_r, sb_s, sb_r,
):
    r = lax.axis_index("row")
    c = lax.axis_index("col")
    core = lax.rem(c, 2)
    chip = lax.div(c, 2)
    partner = c + 1 - 2 * core
    there = (chip, core * 8 + r)
    origin = (lax.rem(c, 8), 2 * r + lax.div(c, 8))
    stays = jnp.logical_and(there[0] == r, there[1] == c)

    def loop(lo, hi, body):
        def run(i, carry):
            body(i)
            return carry

        lax.fori_loop(lo, hi, run, 0)

    def remote(src, dst, ssem, rsem, dev):
        return pltpu.make_async_remote_copy(src, dst, ssem, rsem, device_id=dev, device_id_type=MESH)

    def row_peer(k):
        return lax.rem(r + k, 8)

    def col_peer(k):
        return lax.rem(c + k, 16)

    def block(i):
        return pl.ds(pl.multiple_of(i * B, B), B)

    def load(i):
        return pltpu.make_async_copy(cov.at[pl.ds(i * 256, 256)], cvm.at[pl.ds(i * 256, 256)], csem.at[i])

    loop(0, 8, lambda i: load(i).start())
    barrier = pltpu.get_barrier_semaphore()

    def greet(dev):
        pl.semaphore_signal(barrier, inc=1, device_id=dev, device_id_type=MESH)

    loop(1, 8, lambda k: greet((row_peer(k), c)))
    loop(1, 16, lambda k: greet((r, col_peer(k))))

    @pl.when(jnp.logical_not(stays))
    def _():
        greet(there)
        greet(origin)

    loop(0, 8, lambda i: load(i).wait())

    def gather(i):
        lines = []
        for t in range(8):
            at = seed[i * 8 + t] - r * ROWS
            inside = (at >= 0) & (at < ROWS)
            line = cvm[pl.ds(jnp.clip(at, 0, ROWS - 1), 1), :]
            lines.append(jnp.where(inside, line, 0.0))
        full = jnp.concatenate(lines, axis=0)
        for b in range(8):
            stp[b, pl.ds(pl.multiple_of(i * 8, 8), 8), :] = full[:, b * B : (b + 1) * B]

    loop(0, B // 8, gather)

    @pl.when(stays)
    def _():
        pl.semaphore_wait(barrier, 22)

    @pl.when(jnp.logical_not(stays))
    def _():
        pl.semaphore_wait(barrier, 24)

    def rs1_send(k):
        to = row_peer(k)
        remote(stp.at[to], rs1.at[r], rs1_s.at[to], rs1_r.at[r], (to, c)).start()

    loop(1, 8, rs1_send)

    def split(i):
        high, rest = halves(cvm[block(i), :])
        chi[lax.div(i, 2), lax.rem(i, 2)] = high
        clo[lax.div(i, 2), lax.rem(i, 2)] = rest

    loop(0, 16, split)

    def row_sum(src, dst, ssem, rsem):
        def wait(i):
            @pl.when(i != r)
            def _():
                remote(src.at[i], dst.at[i], ssem.at[i], rsem.at[i], (r, c)).wait_recv()

        loop(0, 8, wait)
        dst[r] = src[r]
        total = dst[0]
        for i in range(1, 8):
            total = total + dst[i]
        return total

    start = row_sum(stp, rs1, rs1_s, rs1_r)
    vcol[:, block(r)] = start
    tsh[0] = start

    def ag1(k):
        return remote(vcol.at[:, block(r)], vcol.at[:, block(r)], ag1_s.at[k], ag1_r.at[r], (row_peer(k), c))

    loop(1, 8, lambda k: ag1(k).start())

    def turn(tag, dst):
        return remote(tsh.at[tag], dst.at[0:B, block(there[1])], t_s.at[tag], t_r.at[tag], there)

    def turn_start(tag, dst):
        @pl.when(jnp.logical_not(stays))
        def _():
            turn(tag, dst).start()

    def turn_wait(tag, dst):
        @pl.when(jnp.logical_not(stays))
        def _():
            remote(tsh.at[tag], dst.at[0:B, block(c)], t_s.at[tag], t_r.at[tag], there).wait_recv()

        @pl.when(stays)
        def _():
            dst[0:B, block(c)] = tsh[tag]

    turn_start(0, st)

    def ag1_wait(k):
        i = row_peer(k)
        remote(vcol.at[:, block(i)], vcol.at[:, block(i)], ag1_s.at[k], ag1_r.at[i], (r, c)).wait_recv()

    loop(1, 8, ag1_wait)

    def gather_start(buf, tag):
        mine = buf.at[0:B, block(c)]

        def send(k):
            i = lax.rem(chip + k, 8)
            remote(mine, mine, ag_s.at[tag, i], ag_r.at[tag, c], (r, 2 * i + core)).start()

        loop(1, 8, send)
        remote(mine, mine, fw_s.at[tag, chip], ag_r.at[tag, c], (r, partner)).start()

    def gather_relay(buf, tag):
        def relay(k):
            i = lax.rem(chip + 8 - k, 8)
            s = 2 * i + core
            got = buf.at[0:B, block(s)]
            remote(got, got, ag_s.at[tag, i], ag_r.at[tag, s], (r, c)).wait_recv()
            remote(got, got, fw_s.at[tag, i], ag_r.at[tag, s], (r, partner)).start()

        loop(1, 8, relay)

    def gather_wait(buf, tag):
        def wait(i):
            s = 2 * i + 1 - core
            got = buf.at[0:B, block(s)]
            remote(got, got, fw_s.at[tag, i], ag_r.at[tag, s], (r, c)).wait_recv()

        loop(0, 8, wait)

    def gather_sent(buf, tag):
        mine = buf.at[0:B, block(c)]

        def wait(i):
            @pl.when(i != chip)
            def _():
                remote(mine, mine, ag_s.at[tag, i], ag_r.at[tag, c], (r, c)).wait_send()

            remote(mine, mine, fw_s.at[tag, i], ag_r.at[tag, c], (r, c)).wait_send()

        loop(0, 8, wait)

    def spread(out, at, n_peers, ssem, rsem, tag, dev):
        loop(1, n_peers, lambda k: remote(out.at[at], out.at[at], ssem.at[tag, k], rsem.at[tag, at], dev(k)).start())

    def collect(out, at, n_peers, ssem, rsem, tag):
        def wait(k):
            i = lax.rem(at + k, n_peers)
            remote(out.at[i], out.at[i], ssem.at[tag, k], rsem.at[tag, i], (r, c)).wait_recv()

        loop(1, n_peers, wait)

    def spread_sent(out, at, n_peers, ssem, rsem, tag):
        loop(1, n_peers, lambda k: remote(out.at[at], out.at[at], ssem.at[tag, k], rsem.at[tag, at], (r, c)).wait_send())

    def over_row(k):
        return (row_peer(k), c)

    def over_col(k):
        return (r, col_peer(k))

    def added(buf, n):
        total = buf[0]
        for i in range(1, n):
            total = total + buf[i]
        return total

    ga[c] = fine(vcol[pl.ds(pl.multiple_of(r * 16, 16), 16), :], vcol[...], NT)
    spread(ga, c, 16, sb_s, sb_r, 0, over_col)

    def cat(i):
        high, rest = halves(vcol[:, block(i)].T)
        scat[block(i), :B] = high
        scat[block(i), B:] = rest

    loop(0, 8, cat)

    def times(first, parity):
        a = chi[pl.ds(first, 4), parity].reshape(512, COLS)
        b = clo[pl.ds(first, 4), parity].reshape(512, COLS)
        full = jnp.dot(a, scat[...], preferred_element_type=F32) + jnp.dot(b, scat[...], preferred_element_type=F32)
        return (full[:, :B] + full[:, B:]).reshape(4, B, B)

    def across(h):
        return remote(ypart.at[pl.ds(h * 4, 4)], d2d.at[pl.ds(h * 4, 4)], d2d_s.at[h], d2d_r.at[h], (r, partner))

    def theirs(h):
        ypart[pl.ds(h * 4, 4)] = times(h * 4, 1 - core)
        across(h).start()

    loop(0, 2, theirs)
    turn_wait(0, st)
    gather_start(st, 0)

    def ours(h):
        yown[pl.ds(h * 4, 4)] = times(h * 4, core)

    loop(0, 2, ours)

    def rs2_copy(i):
        return remote(yown.at[i], rs2.at[chip], rs2_s.at[i], rs2_r.at[chip], (r, 2 * i + core))

    def combine(h):
        across(h).wait_recv()
        for t in range(4):
            i = h * 4 + t
            yown[i] = yown[i] + d2d[i]

            @pl.when(i != chip)
            def _():
                rs2_copy(i).start()

    loop(0, 2, combine)

    collect(ga, c, 16, sb_s, sb_r, 0)
    gb[r] = added(ga, 16)
    spread(gb, r, 8, sa_s, sa_r, 0, over_row)
    gather_relay(st, 0)

    def rs2_wait(i):
        @pl.when(i != chip)
        def _():
            remote(yown.at[i], rs2.at[i], rs2_s.at[i], rs2_r.at[i], (r, c)).wait_recv()

    loop(0, 8, rs2_wait)
    rs2[chip] = yown[chip]
    yt[:, block(c)] = added(rs2, 8).T
    gather_start(yt, 1)

    collect(gb, r, 8, sa_s, sa_r, 0)
    factor(gb[...].reshape(B, B), aug, low0)
    inv0 = low0[:, B:]
    gather_wait(st, 0)

    def put(i):
        return pltpu.make_async_copy(pt.at[pl.ds(i * B, B)], p_out.at[pl.ds(i * B, B)], osem.at[i])

    def first_q(i):
        o = pl.ds(pl.multiple_of(i * 512, 512), 512)
        pt[0:B, o] = fine(inv0, st[:, o])

    loop(0, 4, first_q)
    put(0).start()
    gather_relay(yt, 1)
    gather_wait(yt, 1)

    def small_start(value, buf, tag):
        buf[r] = value
        spread(buf, r, 8, sa_s, sa_r, tag, over_row)

    def small_middle(buf, out, tag):
        collect(buf, r, 8, sa_s, sa_r, tag)
        out[c] = added(buf, 8)
        spread(out, c, 16, sb_s, sb_r, tag, over_col)

    def small_end(out, n, tag):
        collect(out, c, 16, sb_s, sb_r, tag)
        return out[...].reshape(16 * n, B)

    def share(n):
        return pl.ds(pl.multiple_of(c * n, 8), n)

    small_start(fine(pt[share(8), :], yt[...], NT), ha, 1)

    def first_image(i):
        o = pl.ds(pl.multiple_of(i * 512, 512), 512)
        zt[B : 2 * B, o] = fine(inv0, yt[:, o])

    loop(0, 4, first_image)
    first_pass[...] = jnp.zeros((3 * B, 2 * B), F32)
    projection[...] = jnp.zeros((3 * B, 2 * B), F32)
    small_middle(ha, hb, 1)
    h1 = exact(small_end(hb, 8, 1), inv0, NT)
    first_pass[0:B, 0:B] = h1
    h1t = h1.T

    def once(i):
        o = pl.ds(pl.multiple_of(i * 512, 512), 512)
        w = zt[B : 2 * B, o] - fine(h1t, pt[0:B, o])
        pt[B : 2 * B, o] = w
        high, rest = halves(w)
        wt[0:B, o] = high
        wt[B : 2 * B, o] = rest

    loop(0, 4, once)

    def times_t(k):
        q = lax.rem(lax.div(r, 2) + 1 + k, 4)
        o = pl.ds(pl.multiple_of(q * 256, 256), 256)
        a = chi[:, :, :, o].reshape(ROWS, 256)
        b = clo[:, :, :, o].reshape(ROWS, 256)
        full = jnp.dot(wt[...], a, preferred_element_type=F32) + jnp.dot(wt[...], b, preferred_element_type=F32)
        half = full[:B, :] + full[B:, :]
        y1p[2 * q] = half[:, :B]
        y1p[2 * q + 1] = half[:, B:]
        for t in range(2):
            to = 2 * q + t

            @pl.when(to != r)
            def _():
                remote(y1p.at[to], rs3.at[r], rs3_s.at[to], rs3_r.at[r], (to, c)).start()

    loop(0, 4, times_t)

    small_start(fine(pt[share(16), :], pt[B : 2 * B, :], NT), ia, 2)
    tsh[1] = row_sum(y1p, rs3, rs3_s, rs3_r)
    turn_start(1, zt)
    small_middle(ia, ib, 2)
    turn_wait(1, zt)
    gather_start(zt, 2)
    sums = small_end(ib, 16, 2)
    h2 = sums[0:B, :]
    h2t = h2.T
    projection[0:B, 0:B] = h1 + h2
    factor(sums[B : 2 * B, :] - exact(h2, h2, TN), aug, low1)
    projection[B : 2 * B, 0:B] = low1[:, :B]
    inv1 = low1[:, B:]
    gather_relay(zt, 2)

    def second_q(i):
        o = pl.ds(pl.multiple_of(i * 512, 512), 512)
        pt[B : 2 * B, o] = fine(inv1, pt[B : 2 * B, o] - fine(h2t, pt[0:B, o]))

    loop(0, 4, second_q)
    put(1).start()
    mix = jnp.concatenate([inv1, -exact(inv1, h2t)], axis=1)
    gather_wait(zt, 2)

    def image1(i):
        o = pl.ds(pl.multiple_of(i * 512, 512), 512)
        pt[2 * B : 3 * B, o] = fine(mix, zt[:, o])

    loop(0, 4, image1)
    small_start(fine(pt[share(16), :], pt[2 * B : 3 * B, :], NT), ja, 3)
    small_middle(ja, jb, 3)
    h1b = small_end(jb, 16, 3)
    first_pass[0 : 2 * B, B : 2 * B] = h1b
    passed = pltpu.make_async_copy(first_pass, f_out, osem.at[3])
    passed.start()
    h1bt = h1b.T

    def once1(i):
        o = pl.ds(pl.multiple_of(i * 512, 512), 512)
        pt[2 * B : 3 * B, o] = pt[2 * B : 3 * B, o] - fine(h1bt, pt[0 : 2 * B, o])

    loop(0, 4, once1)
    put(2).start()
    small_start(fine(pt[share(24), :], pt[2 * B : 3 * B, :], NT), ka, 4)
    small_middle(ka, kb, 4)
    sums1 = small_end(kb, 24, 4)
    h2b = sums1[0 : 2 * B, :]
    projection[0 : 2 * B, B : 2 * B] = h1b + h2b
    factor(sums1[2 * B : 3 * B, :] - exact(h2b, h2b, TN), aug, low2)
    projection[2 * B : 3 * B, B : 2 * B] = low2[:, :B]
    inv2 = low2[:, B:]
    projected = pltpu.make_async_copy(projection, h_out, osem.at[4])
    projected.start()
    last[...] = jnp.concatenate([-exact(inv2, h2b, NT), inv2], axis=1)
    mixed = pltpu.make_async_copy(last, l_out, osem.at[5])
    mixed.start()

    def sent(i):
        @pl.when(i != r)
        def _():
            remote(stp.at[i], rs1.at[r], rs1_s.at[i], rs1_r.at[r], (r, c)).wait_send()
            remote(y1p.at[i], rs3.at[r], rs3_s.at[i], rs3_r.at[r], (r, c)).wait_send()

        @pl.when(i != chip)
        def _():
            rs2_copy(i).wait_send()

    loop(0, 8, sent)
    loop(1, 8, lambda k: ag1(k).wait_send())

    @pl.when(jnp.logical_not(stays))
    def _():
        turn(0, st).wait_send()
        turn(1, zt).wait_send()

    loop(0, 2, lambda h: across(h).wait_send())
    for tag, buf in enumerate((st, yt, zt)):
        gather_sent(buf, tag)
    spread_sent(ga, c, 16, sb_s, sb_r, 0)
    spread_sent(gb, r, 8, sa_s, sa_r, 0)
    for tag, (a, b) in enumerate(((ha, hb), (ia, ib), (ja, jb), (ka, kb)), 1):
        spread_sent(a, r, 8, sa_s, sa_r, tag)
        spread_sent(b, c, 16, sb_s, sb_r, tag)
    for i in range(3):
        put(i).wait()
    passed.wait()
    projected.wait()
    mixed.wait()


def finish(p, l, h, f, basis, projection, first_pass):
    basis[:, : 2 * B] = p[: 2 * B, :].T * F32(N**0.5)
    basis[:, 2 * B :] = fine(l[...], p[...]).T * F32(N**0.5)
    projection[...] = h[...]
    first_pass[...] = f[...]


def local(covariance, seed_index):
    v = pltpu.VMEM
    dma = pltpu.SemaphoreType.DMA
    blocks8 = v((8, B, B), F32)
    wide = v((B, ROWS), F32)
    square = v((B, 2 * B), F32)
    small = [v((16, 16, B), F32), v((8, 16, B), F32)]
    for n in (8, 16, 16, 24):
        small += [v((8, n, B), F32), v((16, n, B), F32)]
    scratch = [
        v((ROWS, COLS), F32), v((8, 2, B, COLS), BF16), v((8, 2, B, COLS), BF16),
        blocks8, blocks8, v((B, COLS), F32), wide,
        blocks8, blocks8, blocks8, blocks8, wide,
        v((2 * B, ROWS), F32), v((3 * B, ROWS), F32), v((2 * B, ROWS), BF16), blocks8, blocks8, v((2, B, B), F32),
        v((B, 3 * B), F32), v((3 * B, 2 * B), F32), v((3 * B, 2 * B), F32),
        v((COLS, 2 * B), BF16), square, square, square, square, *small,
        dma((8,)), dma((6,)), dma((8,)), dma((8,)), dma((8,)), dma((8,)), dma((2,)), dma((2,)),
        dma((2,)), dma((2,)), dma((8,)), dma((8,)), dma((3, 8)), dma((3, 16)), dma((3, 8)), dma((8,)), dma((8,)),
        dma((5, 8)), dma((5, 8)), dma((5, 16)), dma((5, 16)),
    ]
    any_space = pl.BlockSpec(memory_space=pl.ANY)
    wide_p, mix, square_h, square_f = pl.pallas_call(
        kernel,
        out_shape=(
            jax.ShapeDtypeStruct((3 * B, ROWS), F32),
            jax.ShapeDtypeStruct((B, 3 * B), F32),
            jax.ShapeDtypeStruct((3 * B, 2 * B), F32),
            jax.ShapeDtypeStruct((3 * B, 2 * B), F32),
        ),
        in_specs=[pl.BlockSpec(memory_space=pltpu.SMEM), any_space],
        out_specs=[any_space] * 4,
        scratch_shapes=scratch,
        compiler_params=pltpu.CompilerParams(collective_id=0, has_side_effects=True, vmem_limit_bytes=60 * 2**20),
        name="lanczos",
    )(seed_index, covariance)
    whole = pl.BlockSpec((3 * B, 2 * B), lambda i: (0, 0))
    return pl.pallas_call(
        finish,
        grid=(4,),
        out_shape=(
            jax.ShapeDtypeStruct((ROWS, 3 * B), F32),
            jax.ShapeDtypeStruct((3 * B, 2 * B), F32),
            jax.ShapeDtypeStruct((3 * B, 2 * B), F32),
        ),
        in_specs=[pl.BlockSpec((3 * B, 512), lambda i: (0, i)), pl.BlockSpec((B, 3 * B), lambda i: (0, 0)), whole, whole],
        out_specs=(pl.BlockSpec((512, 3 * B), lambda i: (i, 0)), whole, whole),
        name="finish",
    )(wide_p, mix, square_h, square_f)


def solution(mesh):
    return jax.shard_map(
        local,
        mesh=mesh,
        in_specs=(P("row", "col"), P()),
        out_specs=(P("row", None), P(), P()),
        check_vma=False,
    )
```

```python
import jax
import jax.numpy as jnp
from jax import lax
from jax.experimental import pallas as pl
from jax.experimental.pallas import tpu as pltpu
from jax.sharding import PartitionSpec as P

N = 16384
B = 128
ITERS = 2
ROWS = 2048
COLS = 1024
NB = 16
MESH = pl.DeviceIdType.MESH
F32 = jnp.float32
BF16 = jnp.bfloat16
NN = (((1,), (0,)), ((), ()))
NT = (((1,), (1,)), ((), ()))
TN = (((0,), (0,)), ((), ()))


def exact(a, b, dims=NN):
    return lax.dot_general(a, b, dims, precision=lax.Precision.HIGHEST, preferred_element_type=F32)


def halves(a):
    high = a.astype(BF16)
    return high, (a - high.astype(F32)).astype(BF16)


def fine(a, b, dims=NN):
    ah, al = halves(a)
    bh, bl = halves(b)

    def dot(x, y):
        return lax.dot_general(x, y, dims, preferred_element_type=F32)

    both = dot(jnp.concatenate([ah, al], axis=0), bh)
    n = a.shape[0]
    return both[:n] + (both[n:] + dot(ah, bl))


def factor(gram, aug, low):
    rows = lax.broadcasted_iota(jnp.int32, (B, B), 0)
    lanes = lax.broadcasted_iota(jnp.int32, (B, B), 1)
    aug[:, :B] = gram
    aug[:, B:] = jnp.where(rows == lanes, 1.0, 0.0).astype(F32)
    lane = lax.broadcasted_iota(jnp.int32, (NB, B), 1)
    sub = lax.broadcasted_iota(jnp.int32, (NB, B), 0)

    def panel(p, carry):
        o = pl.multiple_of(p * NB, NB)
        left = aug[pl.ds(o, NB), :B]
        right = aug[pl.ds(o, NB), B:]
        cols = []
        for t in range(NB):
            one = jnp.sum(jnp.where(lane == o + t, left, 0.0), axis=1, keepdims=True)
            cols.append(jnp.broadcast_to(one, (NB, B)))
        for t in range(NB):
            inv = lax.rsqrt(cols[t][t : t + 1, :])
            scale = jnp.where(sub == t, inv, 1.0)
            ratio = jnp.where(sub > t, cols[t] * inv, 0.0)
            left = left * scale
            right = right * scale
            left = left - ratio * left[t : t + 1, :]
            right = right - ratio * right[t : t + 1, :]
            for u in range(t + 1, NB):
                cols[u] = cols[u] - ratio * (cols[u][t : t + 1, :] * inv)
        left = jnp.where(lane >= o, left, 0.0)
        low[pl.ds(o, NB), :B] = jnp.where(lane >= o + sub, left, 0.0)
        low[pl.ds(o, NB), B:] = right
        both = jnp.concatenate([left, right], axis=1)
        aug[...] = aug[...] - exact(left, both, TN)
        return carry

    lax.fori_loop(0, B // NB, panel, 0)


def kernel(
    seed, cov, p_out, l_out, h_out, f_out,
    cvm, chi, clo, stp, rs1, vcol, st, ypart, d2d, yown, rs2, yt, zt, pt, wt, y1p, rs3, tsh, last, projection, first_pass,
    scat, aug, low0, low1, low2, mix, ga, gb, ia, ib, ka, kb, xa1, xb1, xc1, xd1, xa3, xb3, xc3, xd3,
    csem, osem, rs1_s, rs1_r, ag1_s, ag1_r, t_s, t_r, d2d_s, d2d_r, rs2_s, rs2_r, ag_s, ag_r, fw_s, fw_r, rs3_s, rs3_r,
    sa_s, sa_r, sb_s, sb_r, sc_s, sc_r,
):
    r = lax.axis_index("row")
    c = lax.axis_index("col")
    core = lax.rem(c, 2)
    chip = lax.div(c, 2)
    partner = c + 1 - 2 * core
    there = (chip, core * 8 + r)
    origin = (lax.rem(c, 8), 2 * r + lax.div(c, 8))
    stays = jnp.logical_and(there[0] == r, there[1] == c)

    def loop(lo, hi, body):
        def run(i, carry):
            body(i)
            return carry

        lax.fori_loop(lo, hi, run, 0)

    def remote(src, dst, ssem, rsem, dev):
        return pltpu.make_async_remote_copy(src, dst, ssem, rsem, device_id=dev, device_id_type=MESH)

    def row_peer(k):
        return lax.rem(r + k, 8)

    def col_peer(k):
        return lax.rem(c + k, 16)

    def added(buf, n):
        total = buf[0]
        for i in range(1, n):
            total = total + buf[i]
        return total

    def block(i):
        return pl.ds(pl.multiple_of(i * B, B), B)

    def load(i):
        return pltpu.make_async_copy(cov.at[pl.ds(i * 256, 256)], cvm.at[pl.ds(i * 256, 256)], csem.at[0])

    loop(0, 8, lambda i: load(i).start())
    barrier = pltpu.get_barrier_semaphore()

    def greet(dev):
        pl.semaphore_signal(barrier, inc=1, device_id=dev, device_id_type=MESH)

    loop(1, 8, lambda k: greet((row_peer(k), c)))
    loop(1, 16, lambda k: greet((r, col_peer(k))))

    @pl.when(jnp.logical_not(stays))
    def _():
        greet(there)
        greet(origin)

    pltpu.make_async_copy(cov, cvm, csem.at[0]).wait()

    def gather(i):
        lines = []
        for t in range(8):
            at = seed[i * 8 + t] - r * ROWS
            inside = (at >= 0) & (at < ROWS)
            line = cvm[pl.ds(jnp.clip(at, 0, ROWS - 1), 1), :]
            lines.append(jnp.where(inside, line, 0.0))
        full = jnp.concatenate(lines, axis=0)
        for b in range(8):
            stp[b, pl.ds(pl.multiple_of(i * 8, 8), 8), :] = full[:, b * B : (b + 1) * B]

    loop(0, B // 8, gather)

    @pl.when(stays)
    def _():
        pl.semaphore_wait(barrier, 22)

    @pl.when(jnp.logical_not(stays))
    def _():
        pl.semaphore_wait(barrier, 24)

    def rs1_send(k):
        to = row_peer(k)
        remote(stp.at[to], rs1.at[r], rs1_s.at[0], rs1_r.at[0], (to, c)).start()

    loop(1, 8, rs1_send)

    def split(i):
        high, rest = halves(cvm[block(i), :])
        chi[lax.div(i, 2), lax.rem(i, 2)] = high
        clo[lax.div(i, 2), lax.rem(i, 2)] = rest

    loop(0, 16, split)

    def seven(src, dst, ssem, rsem):
        return remote(src.at[pl.ds(0, 7)], dst.at[pl.ds(0, 7)], ssem.at[0], rsem.at[0], (r, c))

    def row_sum(src, dst, ssem, rsem):
        seven(src, dst, ssem, rsem).wait_recv()
        dst[r] = src[r]
        return added(dst, 8)

    start = row_sum(stp, rs1, rs1_s, rs1_r)
    vcol[:, block(r)] = start
    tsh[0] = start

    def ag1(k):
        return remote(vcol.at[:, block(r)], vcol.at[:, block(r)], ag1_s.at[0], ag1_r.at[0], (row_peer(k), c))

    loop(1, 8, lambda k: ag1(k).start())

    def turn(tag, dst, at, dev):
        return remote(tsh.at[tag], dst.at[0:B, block(at)], t_s.at[tag], t_r.at[tag], dev)

    def turn_start(tag, dst):
        @pl.when(jnp.logical_not(stays))
        def _():
            turn(tag, dst, there[1], there).start()

    def turn_wait(tag, dst):
        @pl.when(jnp.logical_not(stays))
        def _():
            turn(tag, dst, c, there).wait_recv()

        @pl.when(stays)
        def _():
            dst[0:B, block(c)] = tsh[tag]

    turn_start(0, st)

    def ag1_all():
        return remote(vcol.at[:, pl.ds(0, 7 * B)], vcol.at[:, pl.ds(0, 7 * B)], ag1_s.at[0], ag1_r.at[0], (r, c))

    ag1_all().wait_recv()

    def gather_start(buf, tag):
        mine = buf.at[0:B, block(c)]

        def send(k):
            i = lax.rem(chip + k, 8)
            remote(mine, mine, ag_s.at[tag], ag_r.at[tag, chip], (r, 2 * i + core)).start()

        loop(1, 8, send)
        remote(mine, mine, fw_s.at[tag], fw_r.at[tag], (r, partner)).start()

    def gather_relay(buf, tag):
        def relay(k):
            i = lax.rem(chip + 8 - k, 8)
            got = buf.at[0:B, block(2 * i + core)]
            remote(got, got, ag_s.at[tag], ag_r.at[tag, i], (r, c)).wait_recv()
            remote(got, got, fw_s.at[tag], fw_r.at[tag], (r, partner)).start()

        loop(1, 8, relay)

    def gather_all(buf, n, ssem, rsem, tag):
        got = buf.at[0:B, pl.ds(0, n * B)]
        return remote(got, got, ssem.at[tag], rsem.at[tag], (r, c))

    def gather_wait(buf, tag):
        gather_all(buf, 8, fw_s, fw_r, tag).wait_recv()

    def gather_sent(buf, tag):
        gather_all(buf, 7, ag_s, fw_r, tag).wait_send()
        gather_all(buf, 8, fw_s, fw_r, tag).wait_send()

    def spread(out, at, n_peers, ssem, rsem, dev):
        loop(1, n_peers, lambda k: remote(out.at[at], out.at[at], ssem, rsem, dev(k)).start())

    def rest(out, n_peers, ssem, rsem):
        got = out.at[pl.ds(0, n_peers - 1)]
        return remote(got, got, ssem, rsem, (r, c))

    def collect(out, n_peers, ssem, rsem):
        rest(out, n_peers, ssem, rsem).wait_recv()

    def over_row(k):
        return (row_peer(k), c)

    def over_col(k):
        return (r, col_peer(k))

    wides = {1: (xa1, xb1, xc1, xd1), 3: (xa3, xb3, xc3, xd3)}

    def wide_start(value, tag):
        a, b = wides[tag][:2]
        a[...] = value.reshape(8, 16, B)

        def send(k):
            to = row_peer(k)
            remote(a.at[to], b.at[r], sa_s.at[tag], sa_r.at[tag], (to, c)).start()

        loop(1, 8, send)

    def wide_second(tag):
        a, b, d = wides[tag][:3]
        collect(b, 8, sa_s.at[tag], sa_r.at[tag])
        b[r] = a[r]
        d[c] = added(b, 8)
        spread(d, c, 16, sb_s.at[tag], sb_r.at[tag], over_col)

    def wide_third(tag):
        d, e = wides[tag][2:]
        collect(d, 16, sb_s.at[tag], sb_r.at[tag])
        e[r] = added(d, 16)
        spread(e, r, 8, sc_s.at[tag], sc_r.at[tag], over_row)

    def wide_end(tag):
        e = wides[tag][3]
        collect(e, 8, sc_s.at[tag], sc_r.at[tag])
        return e[...].reshape(B, B)

    ga[c] = fine(vcol[pl.ds(pl.multiple_of(r * 16, 16), 16), :], vcol[...], NT)
    spread(ga, c, 16, sb_s.at[0], sb_r.at[0], over_col)

    def cat(i):
        high, rest = halves(vcol[:, block(i)].T)
        scat[block(i), :B] = high
        scat[block(i), B:] = rest

    loop(0, 8, cat)

    def times(first, parity):
        a = chi[pl.ds(first, 4), parity].reshape(512, COLS)
        b = clo[pl.ds(first, 4), parity].reshape(512, COLS)
        full = jnp.dot(a, scat[...], preferred_element_type=F32) + jnp.dot(b, scat[...], preferred_element_type=F32)
        return (full[:, :B] + full[:, B:]).reshape(4, B, B)

    def across(h):
        return remote(ypart.at[pl.ds(h * 4, 4)], d2d.at[pl.ds(h * 4, 4)], d2d_s.at[h], d2d_r.at[h], (r, partner))

    def theirs(h):
        ypart[pl.ds(h * 4, 4)] = times(h * 4, 1 - core)
        across(h).start()

    loop(0, 2, theirs)
    turn_wait(0, st)
    gather_start(st, 0)

    def ours(h):
        yown[pl.ds(h * 4, 4)] = times(h * 4, core)

    loop(0, 2, ours)

    def rs2_copy(i):
        return remote(yown.at[i], rs2.at[chip], rs2_s.at[0], rs2_r.at[0], (r, 2 * i + core))

    def combine(h):
        across(h).wait_recv()
        for t in range(4):
            i = h * 4 + t
            yown[i] = yown[i] + d2d[i]

            @pl.when(i != chip)
            def _():
                rs2_copy(i).start()

    loop(0, 2, combine)

    collect(ga, 16, sb_s.at[0], sb_r.at[0])
    gb[r] = added(ga, 16)
    spread(gb, r, 8, sc_s.at[0], sc_r.at[0], over_row)
    gather_relay(st, 0)

    seven(yown, rs2, rs2_s, rs2_r).wait_recv()
    rs2[chip] = yown[chip]
    fresh = added(rs2, 8).T
    yt[:, block(c)] = fresh
    wide_start(exact(st[:, block(c)], fresh, NT), 1)
    gather_start(yt, 1)

    collect(gb, 8, sc_s.at[0], sc_r.at[0])
    factor(gb[...].reshape(B, B), aug, low0)
    inv0 = low0[:, B:]
    wide_second(1)
    gather_wait(st, 0)

    def put(i):
        return pltpu.make_async_copy(pt.at[pl.ds(i * B, B)], p_out.at[pl.ds(i * B, B)], osem.at[0])

    def first_q(i):
        o = pl.ds(pl.multiple_of(i * 512, 512), 512)
        pt[0:B, o] = fine(inv0, st[:, o])

    loop(0, 4, first_q)
    put(0).start()
    gather_relay(yt, 1)
    wide_third(1)
    gather_wait(yt, 1)

    def small_start(value, buf, tag):
        buf[r] = value
        spread(buf, r, 8, sa_s.at[tag], sa_r.at[tag], over_row)

    def small_middle(buf, out, tag):
        collect(buf, 8, sa_s.at[tag], sa_r.at[tag])
        out[c] = added(buf, 8)
        spread(out, c, 16, sb_s.at[tag], sb_r.at[tag], over_col)

    def small_end(out, n, tag):
        collect(out, 16, sb_s.at[tag], sb_r.at[tag])
        return out[...].reshape(16 * n, B)

    def share(n):
        return pl.ds(pl.multiple_of(c * n, 8), n)

    def first_image(i):
        o = pl.ds(pl.multiple_of(i * 512, 512), 512)
        pt[2 * B : 3 * B, o] = fine(inv0, yt[:, o])

    loop(0, 4, first_image)
    first_pass[...] = jnp.zeros((3 * B, 2 * B), F32)
    projection[...] = jnp.zeros((3 * B, 2 * B), F32)
    h1 = exact(exact(inv0, wide_end(1)), inv0, NT)
    first_pass[0:B, 0:B] = h1
    h1t = h1.T

    def once(i):
        o = pl.ds(pl.multiple_of(i * 512, 512), 512)
        w = pt[2 * B : 3 * B, o] - fine(h1t, pt[0:B, o])
        pt[B : 2 * B, o] = w
        high, rest = halves(w)
        wt[0:B, o] = high
        wt[B : 2 * B, o] = rest

    loop(0, 4, once)

    tsh[2] = pt[B : 2 * B, block(c)]

    @pl.when(jnp.logical_not(stays))
    def _():
        remote(tsh.at[2], tsh.at[3], t_s.at[2], t_r.at[2], origin).start()

    def times_t(k):
        q = lax.rem(lax.div(r, 2) + 1 + k, 4)
        o = pl.ds(pl.multiple_of(q * 256, 256), 256)
        a = chi[:, :, :, o].reshape(ROWS, 256)
        b = clo[:, :, :, o].reshape(ROWS, 256)
        full = jnp.dot(wt[...], a, preferred_element_type=F32) + jnp.dot(wt[...], b, preferred_element_type=F32)
        half = full[:B, :] + full[B:, :]
        y1p[2 * q] = half[:, :B]
        y1p[2 * q + 1] = half[:, B:]
        for t in range(2):
            to = 2 * q + t

            @pl.when(to != r)
            def _():
                remote(y1p.at[to], rs3.at[r], rs3_s.at[0], rs3_r.at[0], (to, c)).start()

    loop(0, 4, times_t)

    small_start(fine(pt[share(24), :], pt[B : 2 * B, :], NT), ia, 2)
    fresh1 = row_sum(y1p, rs3, rs3_s, rs3_r)
    tsh[1] = fresh1
    turn_start(1, zt)

    @pl.when(jnp.logical_not(stays))
    def _():
        remote(tsh.at[2], tsh.at[3], t_s.at[2], t_r.at[2], origin).wait_recv()

    @pl.when(stays)
    def _():
        tsh[3] = tsh[2]

    wide_start(exact(tsh[3], tsh[1], NT), 3)
    small_middle(ia, ib, 2)
    wide_second(3)
    turn_wait(1, zt)
    gather_start(zt, 2)
    sums = small_end(ib, 24, 2)
    h2 = sums[0:B, :]
    h2t = h2.T
    crossed = sums[2 * B : 3 * B, :]
    projection[0:B, 0:B] = h1 + h2
    factor(sums[B : 2 * B, :] - exact(h2t, h2), aug, low1)
    projection[B : 2 * B, 0:B] = low1[:, :B]
    inv1 = low1[:, B:]
    wide_third(3)
    tail = exact(inv1, h2t)
    mix1 = jnp.concatenate([-tail, inv1], axis=1)
    gather_relay(zt, 2)

    def second_q(i):
        o = pl.ds(pl.multiple_of(i * 512, 512), 512)
        pt[B : 2 * B, o] = fine(mix1, pt[0 : 2 * B, o])

    loop(0, 4, second_q)
    put(1).start()

    top = exact(crossed - exact(h1t, h2), inv1, NT)
    bent = exact(h2t, crossed - exact(h1, h2) * 0.5)
    below = exact(exact(inv1, wide_end(3) - bent - bent.T), inv1, NT)
    first_pass[0:B, B : 2 * B] = top
    first_pass[B : 2 * B, B : 2 * B] = below
    passed = pltpu.make_async_copy(first_pass, f_out, osem.at[1])
    passed.start()
    mix[...] = jnp.concatenate([inv1, -top.T, -below.T, -tail], axis=1)
    gather_wait(zt, 2)

    def once1(i):
        o = pl.ds(pl.multiple_of(i * 512, 512), 512)
        pt[2 * B : 3 * B, o] = fine(mix[...], jnp.concatenate([zt[:, o], pt[:, o]], axis=0))

    loop(0, 4, once1)
    put(2).start()
    small_start(fine(pt[share(24), :], pt[2 * B : 3 * B, :], NT), ka, 4)
    small_middle(ka, kb, 4)
    sums1 = small_end(kb, 24, 4)
    h2b = sums1[0 : 2 * B, :]
    projection[0:B, B : 2 * B] = top + h2b[0:B]
    projection[B : 2 * B, B : 2 * B] = below + h2b[B:]
    factor(sums1[2 * B : 3 * B, :] - exact(h2b, h2b, TN), aug, low2)
    projection[2 * B : 3 * B, B : 2 * B] = low2[:, :B]
    inv2 = low2[:, B:]
    projected = pltpu.make_async_copy(projection, h_out, osem.at[2])
    projected.start()
    last[...] = jnp.concatenate([-exact(inv2, h2b, NT), inv2], axis=1)
    mixed = pltpu.make_async_copy(last, l_out, osem.at[3])
    mixed.start()

    seven(stp, rs1, rs1_s, rs1_r).wait_send()
    seven(yown, rs2, rs2_s, rs2_r).wait_send()
    seven(y1p, rs3, rs3_s, rs3_r).wait_send()
    ag1_all().wait_send()

    @pl.when(jnp.logical_not(stays))
    def _():
        for tag in range(3):
            turn(tag, zt, c, there).wait_send()

    loop(0, 2, lambda h: across(h).wait_send())
    for tag, buf in enumerate((st, yt, zt)):
        gather_sent(buf, tag)
    rest(ga, 16, sb_s.at[0], sb_r.at[0]).wait_send()
    rest(gb, 8, sc_s.at[0], sc_r.at[0]).wait_send()
    for tag, (a, b) in ((2, (ia, ib)), (4, (ka, kb))):
        rest(a, 8, sa_s.at[tag], sa_r.at[tag]).wait_send()
        rest(b, 16, sb_s.at[tag], sb_r.at[tag]).wait_send()
    for tag in (1, 3):
        rest(wides[tag][0], 8, sa_s.at[tag], sa_r.at[tag]).wait_send()
        rest(wides[tag][2], 16, sb_s.at[tag], sb_r.at[tag]).wait_send()
        rest(wides[tag][3], 8, sc_s.at[tag], sc_r.at[tag]).wait_send()
    pltpu.make_async_copy(pt, p_out, osem.at[0]).wait()
    passed.wait()
    projected.wait()
    mixed.wait()


def finish(p, l, h, f, basis, projection, first_pass):
    basis[:, : 2 * B] = p[: 2 * B, :].T * F32(N**0.5)
    basis[:, 2 * B :] = fine(l[...], p[...]).T * F32(N**0.5)
    projection[...] = h[...]
    first_pass[...] = f[...]


def local(covariance, seed_index):
    v = pltpu.VMEM
    dma = pltpu.SemaphoreType.DMA
    blocks8 = v((8, B, B), F32)
    wide = v((B, ROWS), F32)
    square = v((B, 2 * B), F32)
    small = [v((16, 16, B), F32), v((8, 16, B), F32)]
    for n in (24, 24):
        small += [v((8, n, B), F32), v((16, n, B), F32)]
    thin8, thin16 = v((8, 16, B), F32), v((16, 16, B), F32)
    scratch = [
        v((ROWS, COLS), F32), v((8, 2, B, COLS), BF16), v((8, 2, B, COLS), BF16),
        blocks8, blocks8, v((B, COLS), F32), wide,
        blocks8, blocks8, blocks8, blocks8, wide,
        wide, v((3 * B, ROWS), F32), v((2 * B, ROWS), BF16), blocks8, blocks8, v((4, B, B), F32),
        v((B, 3 * B), F32), v((3 * B, 2 * B), F32), v((3 * B, 2 * B), F32),
        v((COLS, 2 * B), BF16), square, square, square, square, v((B, 4 * B), F32), *small,
        *(thin8, thin8, thin16, thin8) * 2,
        dma((1,)), dma((4,)), dma((1,)), dma((1,)), dma((1,)), dma((1,)), dma((3,)), dma((3,)),
        dma((2,)), dma((2,)), dma((1,)), dma((1,)), dma((3,)), dma((3, 8)), dma((3,)), dma((3,)), dma((1,)), dma((1,)),
        dma((5,)), dma((5,)), dma((5,)), dma((5,)), dma((5,)), dma((5,)),
    ]
    any_space = pl.BlockSpec(memory_space=pl.ANY)
    wide_p, mixed, square_h, square_f = pl.pallas_call(
        kernel,
        out_shape=(
            jax.ShapeDtypeStruct((3 * B, ROWS), F32),
            jax.ShapeDtypeStruct((B, 3 * B), F32),
            jax.ShapeDtypeStruct((3 * B, 2 * B), F32),
            jax.ShapeDtypeStruct((3 * B, 2 * B), F32),
        ),
        in_specs=[pl.BlockSpec(memory_space=pltpu.SMEM), any_space],
        out_specs=[any_space] * 4,
        scratch_shapes=scratch,
        compiler_params=pltpu.CompilerParams(collective_id=0, has_side_effects=True, vmem_limit_bytes=60 * 2**20),
        name="lanczos",
    )(seed_index, covariance)
    whole = pl.BlockSpec((3 * B, 2 * B), lambda i: (0, 0))
    return pl.pallas_call(
        finish,
        grid=(4,),
        out_shape=(
            jax.ShapeDtypeStruct((ROWS, 3 * B), F32),
            jax.ShapeDtypeStruct((3 * B, 2 * B), F32),
            jax.ShapeDtypeStruct((3 * B, 2 * B), F32),
        ),
        in_specs=[pl.BlockSpec((3 * B, 512), lambda i: (0, i)), pl.BlockSpec((B, 3 * B), lambda i: (0, 0)), whole, whole],
        out_specs=(pl.BlockSpec((512, 3 * B), lambda i: (i, 0)), whole, whole),
        name="finish",
    )(wide_p, mixed, square_h, square_f)


def solution(mesh):
    return jax.shard_map(
        local,
        mesh=mesh,
        in_specs=(P("row", "col"), P()),
        out_specs=(P("row", None), P(), P()),
        check_vma=False,
    )
```

```python
import jax
import jax.numpy as jnp
from jax import lax
from jax.experimental import pallas as pl
from jax.experimental.pallas import tpu as pltpu
from jax.sharding import PartitionSpec as P

N = 16384
B = 128
ITERS = 2
ROWS = 2048
COLS = 1024
NB = 16
MESH = pl.DeviceIdType.MESH
F32 = jnp.float32
BF16 = jnp.bfloat16
NN = (((1,), (0,)), ((), ()))
NT = (((1,), (1,)), ((), ()))
TN = (((0,), (0,)), ((), ()))


def exact(a, b, dims=NN):
    return lax.dot_general(a, b, dims, precision=lax.Precision.HIGHEST, preferred_element_type=F32)


def halves(a):
    high = a.astype(BF16)
    return high, (a - high.astype(F32)).astype(BF16)


def fine(a, b, dims=NN):
    ah, al = halves(a)
    bh, bl = halves(b)

    def dot(x, y):
        return lax.dot_general(x, y, dims, preferred_element_type=F32)

    both = dot(jnp.concatenate([ah, al], axis=0), bh)
    n = a.shape[0]
    return both[:n] + (both[n:] + dot(ah, bl))


def factor_start(gram, aug):
    rows = lax.broadcasted_iota(jnp.int32, (B, B), 0)
    lanes = lax.broadcasted_iota(jnp.int32, (B, B), 1)
    aug[:, :B] = gram
    aug[:, B:] = jnp.where(rows == lanes, 1.0, 0.0).astype(F32)


def factor_half(aug, low, half):
    lane = lax.broadcasted_iota(jnp.int32, (NB, B), 1)
    sub = lax.broadcasted_iota(jnp.int32, (NB, B), 0)

    def panel(p, carry):
        o = pl.multiple_of(p * NB, NB)
        left = aug[pl.ds(o, NB), :B]
        right = aug[pl.ds(o, NB), B:]
        cols = []
        for t in range(NB):
            one = jnp.sum(jnp.where(lane == o + t, left, 0.0), axis=1, keepdims=True)
            cols.append(jnp.broadcast_to(one, (NB, B)))
        for t in range(NB):
            inv = lax.rsqrt(cols[t][t : t + 1, :])
            scale = jnp.where(sub == t, inv, 1.0)
            ratio = jnp.where(sub > t, cols[t] * inv, 0.0)
            left = left * scale
            right = right * scale
            left = left - ratio * left[t : t + 1, :]
            right = right - ratio * right[t : t + 1, :]
            for u in range(t + 1, NB):
                cols[u] = cols[u] - ratio * (cols[u][t : t + 1, :] * inv)
        left = jnp.where(lane >= o, left, 0.0)
        low[pl.ds(o, NB), :B] = jnp.where(lane >= o + sub, left, 0.0)
        low[pl.ds(o, NB), B:] = right
        both = jnp.concatenate([left, right], axis=1)
        aug[...] = aug[...] - exact(left, both, TN)
        return carry

    lax.fori_loop(half * (B // NB // 2), (half + 1) * (B // NB // 2), panel, 0)


def kernel(
    seed, cov, p_out, l_out, h_out, f_out,
    cvm, chi, clo, stp, rs1, vcol, st, ypart, d2d, yown, rs2, yt, zt, pt, wt, y1p, rs3, tsh, last, projection, first_pass,
    scat, aug, low0, low1, low2, mix, ga, gb, ia, ib, ka, kb, xa1, xb1, xc1, xd1, xa3, xb3, xc3, xd3,
    csem, osem, rs1_s, rs1_r, ag1_s, ag1_r, t_s, t_r, d2d_s, d2d_r, rs2_s, rs2_r, ag_s, ag_r, fw_s, fw_r, rs3_s, rs3_r,
    sa_s, sa_r, sb_s, sb_r, sc_s, sc_r,
):
    r = lax.axis_index("row")
    c = lax.axis_index("col")
    core = lax.rem(c, 2)
    chip = lax.div(c, 2)
    partner = c + 1 - 2 * core
    there = (chip, core * 8 + r)
    origin = (lax.rem(c, 8), 2 * r + lax.div(c, 8))
    stays = jnp.logical_and(there[0] == r, there[1] == c)

    def loop(lo, hi, body):
        def run(i, carry):
            body(i)
            return carry

        lax.fori_loop(lo, hi, run, 0)

    def remote(src, dst, ssem, rsem, dev):
        return pltpu.make_async_remote_copy(src, dst, ssem, rsem, device_id=dev, device_id_type=MESH)

    def row_peer(k):
        return lax.rem(r + k, 8)

    def col_peer(k):
        return lax.rem(c + k, 16)

    def added(buf, n):
        total = buf[0]
        for i in range(1, n):
            total = total + buf[i]
        return total

    def block(i):
        return pl.ds(pl.multiple_of(i * B, B), B)

    def load(i):
        return pltpu.make_async_copy(cov.at[pl.ds(i * 256, 256)], cvm.at[pl.ds(i * 256, 256)], csem.at[0])

    loop(0, 8, lambda i: load(i).start())
    barrier = pltpu.get_barrier_semaphore()

    def greet(dev):
        pl.semaphore_signal(barrier, inc=1, device_id=dev, device_id_type=MESH)

    loop(1, 8, lambda k: greet((row_peer(k), c)))
    loop(1, 16, lambda k: greet((r, col_peer(k))))

    @pl.when(jnp.logical_not(stays))
    def _():
        greet(there)
        greet(origin)

    pltpu.make_async_copy(cov, cvm, csem.at[0]).wait()

    def gather(i):
        lines = []
        for t in range(8):
            at = seed[i * 8 + t] - r * ROWS
            inside = (at >= 0) & (at < ROWS)
            line = cvm[pl.ds(jnp.clip(at, 0, ROWS - 1), 1), :]
            lines.append(jnp.where(inside, line, 0.0))
        full = jnp.concatenate(lines, axis=0)
        for b in range(8):
            stp[b, pl.ds(pl.multiple_of(i * 8, 8), 8), :] = full[:, b * B : (b + 1) * B]

    loop(0, B // 8, gather)

    @pl.when(stays)
    def _():
        pl.semaphore_wait(barrier, 22)

    @pl.when(jnp.logical_not(stays))
    def _():
        pl.semaphore_wait(barrier, 24)

    def rs1_send(k):
        to = row_peer(k)
        remote(stp.at[to], rs1.at[r], rs1_s.at[0], rs1_r.at[0], (to, c)).start()

    loop(1, 8, rs1_send)

    def split(i):
        high, rest = halves(cvm[block(i), :])
        chi[lax.div(i, 2), lax.rem(i, 2)] = high
        clo[lax.div(i, 2), lax.rem(i, 2)] = rest

    loop(0, 16, split)

    def seven(src, dst, ssem, rsem):
        return remote(src.at[pl.ds(0, 7)], dst.at[pl.ds(0, 7)], ssem.at[0], rsem.at[0], (r, c))

    def row_sum(src, dst, ssem, rsem):
        seven(src, dst, ssem, rsem).wait_recv()
        dst[r] = src[r]
        return added(dst, 8)

    start = row_sum(stp, rs1, rs1_s, rs1_r)
    vcol[:, block(r)] = start
    tsh[0] = start

    def ag1(k):
        return remote(vcol.at[:, block(r)], vcol.at[:, block(r)], ag1_s.at[0], ag1_r.at[0], (row_peer(k), c))


    def turn(tag, dst, at, dev):
        return remote(tsh.at[tag], dst.at[0:B, block(at)], t_s.at[tag], t_r.at[tag], dev)

    def turn_start(tag, dst):
        @pl.when(jnp.logical_not(stays))
        def _():
            turn(tag, dst, there[1], there).start()

    def turn_wait(tag, dst):
        @pl.when(jnp.logical_not(stays))
        def _():
            turn(tag, dst, c, there).wait_recv()

        @pl.when(stays)
        def _():
            dst[0:B, block(c)] = tsh[tag]


    def ag1_all():
        return remote(vcol.at[:, pl.ds(0, 7 * B)], vcol.at[:, pl.ds(0, 7 * B)], ag1_s.at[0], ag1_r.at[0], (r, c))


    def gather_start(buf, tag):
        mine = buf.at[0:B, block(c)]

        def send(k):
            i = lax.rem(chip + k, 8)
            remote(mine, mine, ag_s.at[tag], ag_r.at[tag, chip], (r, 2 * i + core)).start()

        loop(1, 8, send)
        remote(mine, mine, fw_s.at[tag], fw_r.at[tag], (r, partner)).start()

    def gather_relay(buf, tag):
        def relay(k):
            i = lax.rem(chip + 8 - k, 8)
            got = buf.at[0:B, block(2 * i + core)]
            remote(got, got, ag_s.at[tag], ag_r.at[tag, i], (r, c)).wait_recv()
            remote(got, got, fw_s.at[tag], fw_r.at[tag], (r, partner)).start()

        loop(1, 8, relay)

    def gather_all(buf, n, ssem, rsem, tag):
        got = buf.at[0:B, pl.ds(0, n * B)]
        return remote(got, got, ssem.at[tag], rsem.at[tag], (r, c))

    def gather_wait(buf, tag):
        gather_all(buf, 8, fw_s, fw_r, tag).wait_recv()

    def gather_sent(buf, tag):
        gather_all(buf, 7, ag_s, fw_r, tag).wait_send()
        gather_all(buf, 8, fw_s, fw_r, tag).wait_send()

    def spread(out, at, n_peers, ssem, rsem, dev):
        loop(1, n_peers, lambda k: remote(out.at[at], out.at[at], ssem, rsem, dev(k)).start())

    def rest(out, n_peers, ssem, rsem):
        got = out.at[pl.ds(0, n_peers - 1)]
        return remote(got, got, ssem, rsem, (r, c))

    def collect(out, n_peers, ssem, rsem):
        rest(out, n_peers, ssem, rsem).wait_recv()

    def over_row(k):
        return (row_peer(k), c)

    def over_col(k):
        return (r, col_peer(k))

    wides = {1: (xa1, xb1, xc1, xd1), 3: (xa3, xb3, xc3, xd3)}

    def wide_start(value, tag):
        a, b = wides[tag][:2]
        a[...] = value.reshape(8, 16, B)

        def send(k):
            to = row_peer(k)
            remote(a.at[to], b.at[r], sa_s.at[tag], sa_r.at[tag], (to, c)).start()

        loop(1, 8, send)

    def wide_second(tag):
        a, b, d = wides[tag][:3]
        collect(b, 8, sa_s.at[tag], sa_r.at[tag])
        b[r] = a[r]
        d[c] = added(b, 8)
        spread(d, c, 16, sb_s.at[tag], sb_r.at[tag], over_col)

    def wide_third(tag):
        d, e = wides[tag][2:]
        collect(d, 16, sb_s.at[tag], sb_r.at[tag])
        e[r] = added(d, 16)
        spread(e, r, 8, sc_s.at[tag], sc_r.at[tag], over_row)

    def wide_end(tag):
        e = wides[tag][3]
        collect(e, 8, sc_s.at[tag], sc_r.at[tag])
        return e[...].reshape(B, B)

    turn_start(0, st)
    loop(1, 8, lambda k: ag1(k).start())
    turn_wait(0, st)
    gather_start(st, 0)
    ag1_all().wait_recv()

    ga[c] = fine(vcol[pl.ds(pl.multiple_of(r * 16, 16), 16), :], vcol[...], NT)
    spread(ga, c, 16, sb_s.at[0], sb_r.at[0], over_col)

    def cat(i):
        high, rest = halves(vcol[:, block(i)].T)
        scat[block(i), :B] = high
        scat[block(i), B:] = rest

    loop(0, 8, cat)

    def times(first, parity):
        a = chi[pl.ds(first, 4), parity].reshape(512, COLS)
        b = clo[pl.ds(first, 4), parity].reshape(512, COLS)
        full = jnp.dot(a, scat[...], preferred_element_type=F32) + jnp.dot(b, scat[...], preferred_element_type=F32)
        return (full[:, :B] + full[:, B:]).reshape(4, B, B)

    def across(h):
        return remote(ypart.at[pl.ds(h * 4, 4)], d2d.at[pl.ds(h * 4, 4)], d2d_s.at[h], d2d_r.at[h], (r, partner))

    def theirs(h):
        ypart[pl.ds(h * 4, 4)] = times(h * 4, 1 - core)
        across(h).start()

    loop(0, 2, theirs)

    def ours(h):
        yown[pl.ds(h * 4, 4)] = times(h * 4, core)

    loop(0, 2, ours)

    def rs2_copy(i):
        return remote(yown.at[i], rs2.at[chip], rs2_s.at[0], rs2_r.at[0], (r, 2 * i + core))

    def combine(h):
        across(h).wait_recv()
        for t in range(4):
            i = h * 4 + t
            yown[i] = yown[i] + d2d[i]

            @pl.when(i != chip)
            def _():
                rs2_copy(i).start()

    loop(0, 2, combine)

    gather_relay(st, 0)
    gather_wait(st, 0)

    bent0 = fine(st[:, block(core)], yown[0])
    for i in range(1, 8):
        bent0 = bent0 + fine(st[:, block(2 * i + core)], yown[i])
    wide_start(bent0, 1)

    collect(ga, 16, sb_s.at[0], sb_r.at[0])
    gb[r] = added(ga, 16)
    spread(gb, r, 8, sc_s.at[0], sc_r.at[0], over_row)

    seven(yown, rs2, rs2_s, rs2_r).wait_recv()
    rs2[chip] = yown[chip]
    yt[:, block(c)] = added(rs2, 8).T
    wide_second(1)
    gather_start(yt, 1)

    collect(gb, 8, sc_s.at[0], sc_r.at[0])
    factor_start(gb[...].reshape(B, B), aug)
    factor_half(aug, low0, 0)
    factor_half(aug, low0, 1)
    wide_third(1)
    inv0 = low0[:, B:]

    def put(i):
        return pltpu.make_async_copy(pt.at[pl.ds(i * B, B)], p_out.at[pl.ds(i * B, B)], osem.at[0])

    def first_q(i):
        o = pl.ds(i * 512, 512)
        pt[0:B, o] = fine(inv0, st[:, o])

    for i in range(4):
        first_q(i)

    put(0).start()
    gather_relay(yt, 1)
    gather_wait(yt, 1)

    def small_start(value, buf, tag):
        buf[r] = value
        spread(buf, r, 8, sa_s.at[tag], sa_r.at[tag], over_row)

    def small_middle(buf, out, tag):
        collect(buf, 8, sa_s.at[tag], sa_r.at[tag])
        out[c] = added(buf, 8)
        spread(out, c, 16, sb_s.at[tag], sb_r.at[tag], over_col)

    def small_end(out, n, tag):
        collect(out, 16, sb_s.at[tag], sb_r.at[tag])
        return out[...].reshape(16 * n, B)

    def share(n):
        return pl.ds(pl.multiple_of(c * n, 8), n)

    def first_image(i):
        o = pl.ds(i * 512, 512)
        pt[2 * B : 3 * B, o] = fine(inv0, yt[:, o])

    for i in range(4):
        first_image(i)

    first_pass[...] = jnp.zeros((3 * B, 2 * B), F32)
    projection[...] = jnp.zeros((3 * B, 2 * B), F32)
    h1 = exact(exact(inv0, wide_end(1)), inv0, NT)
    first_pass[0:B, 0:B] = h1
    h1t = h1.T

    def once(i):
        o = pl.ds(i * 512, 512)
        w = pt[2 * B : 3 * B, o] - fine(h1t, pt[0:B, o])
        pt[B : 2 * B, o] = w
        high, rest = halves(w)
        wt[0:B, o] = high
        wt[B : 2 * B, o] = rest

    for i in range(4):
        once(i)


    tsh[2] = pt[B : 2 * B, block(c)]

    @pl.when(jnp.logical_not(stays))
    def _():
        remote(tsh.at[2], tsh.at[3], t_s.at[2], t_r.at[2], origin).start()

    def times_t(k):
        q = lax.rem(lax.div(r, 2) + 1 + k, 4)
        o = pl.ds(pl.multiple_of(q * 256, 256), 256)
        a = chi[:, :, :, o].reshape(ROWS, 256)
        b = clo[:, :, :, o].reshape(ROWS, 256)
        full = jnp.dot(wt[...], a, preferred_element_type=F32) + jnp.dot(wt[...], b, preferred_element_type=F32)
        half = full[:B, :] + full[B:, :]
        y1p[2 * q] = half[:, :B]
        y1p[2 * q + 1] = half[:, B:]
        for t in range(2):
            to = 2 * q + t

            @pl.when(to != r)
            def _():
                remote(y1p.at[to], rs3.at[r], rs3_s.at[0], rs3_r.at[0], (to, c)).start()

    loop(0, 4, times_t)

    small_start(fine(pt[share(24), :], pt[B : 2 * B, :], NT), ia, 2)
    fresh1 = row_sum(y1p, rs3, rs3_s, rs3_r)
    tsh[1] = fresh1
    turn_start(1, zt)

    @pl.when(jnp.logical_not(stays))
    def _():
        remote(tsh.at[2], tsh.at[3], t_s.at[2], t_r.at[2], origin).wait_recv()

    @pl.when(stays)
    def _():
        tsh[3] = tsh[2]

    wide_start(exact(tsh[3], tsh[1], NT), 3)
    small_middle(ia, ib, 2)
    wide_second(3)
    turn_wait(1, zt)
    gather_start(zt, 2)
    sums = small_end(ib, 24, 2)
    h2 = sums[0:B, :]
    h2t = h2.T
    crossed = sums[2 * B : 3 * B, :]
    projection[0:B, 0:B] = h1 + h2
    factor_start(sums[B : 2 * B, :] - exact(h2t, h2), aug)
    factor_half(aug, low1, 0)
    wide_third(3)
    factor_half(aug, low1, 1)
    projection[B : 2 * B, 0:B] = low1[:, :B]
    inv1 = low1[:, B:]
    tail = exact(inv1, h2t)
    mix1 = jnp.concatenate([-tail, inv1], axis=1)

    def second_q(i):
        o = pl.ds(i * 512, 512)
        pt[B : 2 * B, o] = fine(mix1, pt[0 : 2 * B, o])

    for i in range(4):
        second_q(i)

    put(1).start()

    top = exact(crossed - exact(h1t, h2), inv1, NT)
    bent = exact(h2t, crossed - exact(h1, h2) * 0.5)
    first_pass[0:B, B : 2 * B] = top
    gather_relay(zt, 2)
    below = exact(exact(inv1, wide_end(3) - bent - bent.T), inv1, NT)
    first_pass[B : 2 * B, B : 2 * B] = below
    passed = pltpu.make_async_copy(first_pass, f_out, osem.at[1])
    passed.start()
    mix[...] = jnp.concatenate([inv1, -top.T, -below.T, -tail], axis=1)
    gather_wait(zt, 2)

    def once1(i):
        o = pl.ds(i * 512, 512)
        pt[2 * B : 3 * B, o] = fine(mix[...], jnp.concatenate([zt[:, o], pt[:, o]], axis=0))

    for i in range(4):
        once1(i)

    put(2).start()
    small_start(fine(pt[share(24), :], pt[2 * B : 3 * B, :], NT), ka, 4)
    small_middle(ka, kb, 4)
    sums1 = small_end(kb, 24, 4)
    h2b = sums1[0 : 2 * B, :]
    projection[0:B, B : 2 * B] = top + h2b[0:B]
    projection[B : 2 * B, B : 2 * B] = below + h2b[B:]
    factor_start(sums1[2 * B : 3 * B, :] - exact(h2b, h2b, TN), aug)
    factor_half(aug, low2, 0)
    factor_half(aug, low2, 1)
    projection[2 * B : 3 * B, B : 2 * B] = low2[:, :B]
    inv2 = low2[:, B:]
    projected = pltpu.make_async_copy(projection, h_out, osem.at[2])
    projected.start()
    last[...] = jnp.concatenate([-exact(inv2, h2b, NT), inv2], axis=1)
    mixed = pltpu.make_async_copy(last, l_out, osem.at[3])
    mixed.start()

    seven(stp, rs1, rs1_s, rs1_r).wait_send()
    seven(yown, rs2, rs2_s, rs2_r).wait_send()
    seven(y1p, rs3, rs3_s, rs3_r).wait_send()
    ag1_all().wait_send()

    @pl.when(jnp.logical_not(stays))
    def _():
        for tag in range(3):
            turn(tag, zt, c, there).wait_send()

    loop(0, 2, lambda h: across(h).wait_send())
    for tag, buf in enumerate((st, yt, zt)):
        gather_sent(buf, tag)
    rest(ga, 16, sb_s.at[0], sb_r.at[0]).wait_send()
    rest(gb, 8, sc_s.at[0], sc_r.at[0]).wait_send()
    for tag, (a, b) in ((2, (ia, ib)), (4, (ka, kb))):
        rest(a, 8, sa_s.at[tag], sa_r.at[tag]).wait_send()
        rest(b, 16, sb_s.at[tag], sb_r.at[tag]).wait_send()
    for tag in (1, 3):
        rest(wides[tag][0], 8, sa_s.at[tag], sa_r.at[tag]).wait_send()
        rest(wides[tag][2], 16, sb_s.at[tag], sb_r.at[tag]).wait_send()
        rest(wides[tag][3], 8, sc_s.at[tag], sc_r.at[tag]).wait_send()
    pltpu.make_async_copy(pt, p_out, osem.at[0]).wait()
    passed.wait()
    projected.wait()
    mixed.wait()


def finish(p, l, h, f, basis, projection, first_pass):
    basis[:, : 2 * B] = p[: 2 * B, :].T * F32(N**0.5)
    basis[:, 2 * B :] = fine(l[...], p[...]).T * F32(N**0.5)
    projection[...] = h[...]
    first_pass[...] = f[...]


def local(covariance, seed_index):
    v = pltpu.VMEM
    dma = pltpu.SemaphoreType.DMA
    blocks8 = v((8, B, B), F32)
    wide = v((B, ROWS), F32)
    square = v((B, 2 * B), F32)
    small = [v((16, 16, B), F32), v((8, 16, B), F32)]
    for n in (24, 24):
        small += [v((8, n, B), F32), v((16, n, B), F32)]
    thin8, thin16 = v((8, 16, B), F32), v((16, 16, B), F32)
    scratch = [
        v((ROWS, COLS), F32), v((8, 2, B, COLS), BF16), v((8, 2, B, COLS), BF16),
        blocks8, blocks8, v((B, COLS), F32), wide,
        blocks8, blocks8, blocks8, blocks8, wide,
        wide, v((3 * B, ROWS), F32), v((2 * B, ROWS), BF16), blocks8, blocks8, v((4, B, B), F32),
        v((B, 3 * B), F32), v((3 * B, 2 * B), F32), v((3 * B, 2 * B), F32),
        v((COLS, 2 * B), BF16), square, square, square, square, v((B, 4 * B), F32), *small,
        *(thin8, thin8, thin16, thin8) * 2,
        dma((1,)), dma((4,)), dma((1,)), dma((1,)), dma((1,)), dma((1,)), dma((3,)), dma((3,)),
        dma((2,)), dma((2,)), dma((1,)), dma((1,)), dma((3,)), dma((3, 8)), dma((3,)), dma((3,)), dma((1,)), dma((1,)),
        dma((5,)), dma((5,)), dma((5,)), dma((5,)), dma((5,)), dma((5,)),
    ]
    any_space = pl.BlockSpec(memory_space=pl.ANY)
    wide_p, mixed, square_h, square_f = pl.pallas_call(
        kernel,
        out_shape=(
            jax.ShapeDtypeStruct((3 * B, ROWS), F32),
            jax.ShapeDtypeStruct((B, 3 * B), F32),
            jax.ShapeDtypeStruct((3 * B, 2 * B), F32),
            jax.ShapeDtypeStruct((3 * B, 2 * B), F32),
        ),
        in_specs=[pl.BlockSpec(memory_space=pltpu.SMEM), any_space],
        out_specs=[any_space] * 4,
        scratch_shapes=scratch,
        compiler_params=pltpu.CompilerParams(collective_id=0, has_side_effects=True, vmem_limit_bytes=60 * 2**20),
        name="lanczos",
    )(seed_index, covariance)
    whole = pl.BlockSpec((3 * B, 2 * B), lambda i: (0, 0))
    return pl.pallas_call(
        finish,
        grid=(2,),
        out_shape=(
            jax.ShapeDtypeStruct((ROWS, 3 * B), F32),
            jax.ShapeDtypeStruct((3 * B, 2 * B), F32),
            jax.ShapeDtypeStruct((3 * B, 2 * B), F32),
        ),
        in_specs=[pl.BlockSpec((3 * B, ROWS // 2), lambda i: (0, i)), pl.BlockSpec((B, 3 * B), lambda i: (0, 0)), whole, whole],
        out_specs=(pl.BlockSpec((ROWS // 2, 3 * B), lambda i: (i, 0)), whole, whole),
        name="finish",
    )(wide_p, mixed, square_h, square_f)


def solution(mesh):
    return jax.shard_map(
        local,
        mesh=mesh,
        in_specs=(P("row", "col"), P()),
        out_specs=(P("row", None), P(), P()),
        check_vma=False,
    )
```

```python
import jax
import jax.numpy as jnp
from jax import lax
from jax.experimental import pallas as pl
from jax.experimental.pallas import tpu as pltpu
from jax.sharding import PartitionSpec as P

N = 16384
B = 128
ITERS = 2
ROWS = 2048
COLS = 1024
NB = 16
MESH = pl.DeviceIdType.MESH
F32 = jnp.float32
BF16 = jnp.bfloat16
NN = (((1,), (0,)), ((), ()))
NT = (((1,), (1,)), ((), ()))
TN = (((0,), (0,)), ((), ()))


def halves(a):
    high = a.astype(BF16)
    return high, (a - high.astype(F32)).astype(BF16)


def exact(a, b, dims=NN):
    def thirds(x):
        high = x.astype(BF16)
        rest = x - high.astype(F32)
        middle = rest.astype(BF16)
        return high, middle, (rest - middle.astype(F32)).astype(BF16)

    (over_a,), (over_b,) = dims[0]
    ah, am, al = thirds(a)
    bh, bm, bl = thirds(b)
    left = jnp.concatenate([al, am, ah, am, ah, ah], axis=over_a)
    right = jnp.concatenate([bh, bm, bl, bh, bm, bh], axis=over_b)
    return lax.dot_general(left, right, dims, preferred_element_type=F32)


def fine(a, b, dims=NN):
    ah, al = halves(a)
    bh, bl = halves(b)

    def dot(x, y):
        return lax.dot_general(x, y, dims, preferred_element_type=F32)

    both = dot(jnp.concatenate([ah, al], axis=0), bh)
    n = a.shape[0]
    return both[:n] + (both[n:] + dot(ah, bl))


def factor_start(gram, aug):
    rows = lax.broadcasted_iota(jnp.int32, (B, B), 0)
    lanes = lax.broadcasted_iota(jnp.int32, (B, B), 1)
    aug[:, :B] = gram
    aug[:, B:] = jnp.where(rows == lanes, 1.0, 0.0).astype(F32)


def factor_half(aug, low, half):
    lane = lax.broadcasted_iota(jnp.int32, (NB, B), 1)
    sub = lax.broadcasted_iota(jnp.int32, (NB, B), 0)

    def panel(p, carry):
        o = pl.multiple_of(p * NB, NB)
        left = aug[pl.ds(o, NB), :B]
        right = aug[pl.ds(o, NB), B:]
        cols = []
        for t in range(NB):
            one = jnp.sum(jnp.where(lane == o + t, left, 0.0), axis=1, keepdims=True)
            cols.append(jnp.broadcast_to(one, (NB, B)))
        for t in range(NB):
            inv = lax.rsqrt(cols[t][t : t + 1, :])
            scale = jnp.where(sub == t, inv, 1.0)
            ratio = jnp.where(sub > t, cols[t] * inv, 0.0)
            left = left * scale
            right = right * scale
            left = left - ratio * left[t : t + 1, :]
            right = right - ratio * right[t : t + 1, :]
            for u in range(t + 1, NB):
                cols[u] = cols[u] - ratio * (cols[u][t : t + 1, :] * inv)
        left = jnp.where(lane >= o, left, 0.0)
        low[pl.ds(o, NB), :B] = jnp.where(lane >= o + sub, left, 0.0)
        low[pl.ds(o, NB), B:] = right
        both = jnp.concatenate([left, right], axis=1)
        aug[...] = aug[...] - exact(left, both, TN)
        return carry

    lax.fori_loop(half * (B // NB // 2), (half + 1) * (B // NB // 2), panel, 0)


def kernel(
    seed, cov, p_out, l_out, h_out, f_out,
    cvm, chi, clo, stp, rs1, vcol, st, ypart, d2d, yown, rs2, yt, zt, pt, wt, y1p, rs3, tsh, last, projection, first_pass,
    scat, aug, low0, low1, low2, mix, ga, gb, ia, ib, ka, kb, xa1, xb1, xc1, xd1, xa3, xb3, xc3, xd3,
    csem, osem, rs1_s, rs1_r, ag1_s, ag1_r, t_s, t_r, d2d_s, d2d_r, rs2_s, rs2_r, ag_s, ag_r, fw_s, fw_r, rs3_s, rs3_r,
    sa_s, sa_r, sb_s, sb_r, sc_s, sc_r,
):
    r = lax.axis_index("row")
    c = lax.axis_index("col")
    core = lax.rem(c, 2)
    chip = lax.div(c, 2)
    partner = c + 1 - 2 * core
    there = (chip, core * 8 + r)
    origin = (lax.rem(c, 8), 2 * r + lax.div(c, 8))
    stays = jnp.logical_and(there[0] == r, there[1] == c)

    def loop(lo, hi, body):
        def run(i, carry):
            body(i)
            return carry

        lax.fori_loop(lo, hi, run, 0)

    def remote(src, dst, ssem, rsem, dev):
        return pltpu.make_async_remote_copy(src, dst, ssem, rsem, device_id=dev, device_id_type=MESH)

    def row_peer(k):
        return lax.rem(r + k, 8)

    def col_peer(k):
        return lax.rem(c + k, 16)

    def added(buf, n):
        total = buf[0]
        for i in range(1, n):
            total = total + buf[i]
        return total

    def block(i):
        return pl.ds(pl.multiple_of(i * B, B), B)

    def load(i):
        return pltpu.make_async_copy(cov.at[pl.ds(i * 256, 256)], cvm.at[pl.ds(i * 256, 256)], csem.at[0])

    loop(0, 8, lambda i: load(i).start())
    barrier = pltpu.get_barrier_semaphore()

    def greet(dev):
        pl.semaphore_signal(barrier, inc=1, device_id=dev, device_id_type=MESH)

    loop(1, 8, lambda k: greet((row_peer(k), c)))
    loop(1, 16, lambda k: greet((r, col_peer(k))))

    @pl.when(jnp.logical_not(stays))
    def _():
        greet(there)
        greet(origin)

    pltpu.make_async_copy(cov, cvm, csem.at[0]).wait()

    def gather(i):
        lines = []
        for t in range(8):
            at = seed[i * 8 + t] - r * ROWS
            inside = (at >= 0) & (at < ROWS)
            line = cvm[pl.ds(jnp.clip(at, 0, ROWS - 1), 1), :]
            lines.append(jnp.where(inside, line, 0.0))
        full = jnp.concatenate(lines, axis=0)
        for b in range(8):
            stp[b, pl.ds(pl.multiple_of(i * 8, 8), 8), :] = full[:, b * B : (b + 1) * B]

    loop(0, B // 8, gather)

    @pl.when(stays)
    def _():
        pl.semaphore_wait(barrier, 22)

    @pl.when(jnp.logical_not(stays))
    def _():
        pl.semaphore_wait(barrier, 24)

    def rs1_send(k):
        to = row_peer(k)
        remote(stp.at[to], rs1.at[r], rs1_s.at[0], rs1_r.at[0], (to, c)).start()

    loop(1, 8, rs1_send)

    def split(i):
        high, rest = halves(cvm[block(i), :])
        chi[lax.div(i, 2), lax.rem(i, 2)] = high
        clo[lax.div(i, 2), lax.rem(i, 2)] = rest

    loop(0, 16, split)

    def seven(src, dst, ssem, rsem):
        return remote(src.at[pl.ds(0, 7)], dst.at[pl.ds(0, 7)], ssem.at[0], rsem.at[0], (r, c))

    def row_sum(src, dst, ssem, rsem):
        seven(src, dst, ssem, rsem).wait_recv()
        dst[r] = src[r]
        return added(dst, 8)

    start = row_sum(stp, rs1, rs1_s, rs1_r)
    vcol[:, block(r)] = start
    tsh[0] = start

    def ag1(k):
        return remote(vcol.at[:, block(r)], vcol.at[:, block(r)], ag1_s.at[0], ag1_r.at[r], (row_peer(k), c))


    def turn(tag, dst, at, dev):
        return remote(tsh.at[tag], dst.at[0:B, block(at)], t_s.at[tag], t_r.at[tag], dev)

    def turn_start(tag, dst):
        @pl.when(jnp.logical_not(stays))
        def _():
            turn(tag, dst, there[1], there).start()

    def turn_wait(tag, dst):
        @pl.when(jnp.logical_not(stays))
        def _():
            turn(tag, dst, c, there).wait_recv()

        @pl.when(stays)
        def _():
            dst[0:B, block(c)] = tsh[tag]


    def ag1_sent():
        return remote(vcol.at[:, pl.ds(0, 7 * B)], vcol.at[:, pl.ds(0, 7 * B)], ag1_s.at[0], ag1_r.at[0], (r, c))

    def gather_start(buf, tag):
        mine = buf.at[0:B, block(c)]

        def send(k):
            i = lax.rem(chip + k, 8)
            remote(mine, mine, ag_s.at[tag], ag_r.at[tag, chip], (r, 2 * i + core)).start()

        loop(1, 8, send)
        remote(mine, mine, fw_s.at[tag], fw_r.at[tag], (r, partner)).start()

    def gather_relay(buf, tag):
        def relay(k):
            i = lax.rem(chip + 8 - k, 8)
            got = buf.at[0:B, block(2 * i + core)]
            remote(got, got, ag_s.at[tag], ag_r.at[tag, i], (r, c)).wait_recv()
            remote(got, got, fw_s.at[tag], fw_r.at[tag], (r, partner)).start()

        loop(1, 8, relay)

    def gather_all(buf, n, ssem, rsem, tag):
        got = buf.at[0:B, pl.ds(0, n * B)]
        return remote(got, got, ssem.at[tag], rsem.at[tag], (r, c))

    def gather_wait(buf, tag):
        gather_all(buf, 8, fw_s, fw_r, tag).wait_recv()

    def gather_sent(buf, tag):
        gather_all(buf, 7, ag_s, fw_r, tag).wait_send()
        gather_all(buf, 8, fw_s, fw_r, tag).wait_send()

    def spread(out, at, n_peers, ssem, rsem, dev):
        loop(1, n_peers, lambda k: remote(out.at[at], out.at[at], ssem, rsem, dev(k)).start())

    def rest(out, n_peers, ssem, rsem):
        got = out.at[pl.ds(0, n_peers - 1)]
        return remote(got, got, ssem, rsem, (r, c))

    def collect(out, n_peers, ssem, rsem):
        rest(out, n_peers, ssem, rsem).wait_recv()

    def over_row(k):
        return (row_peer(k), c)

    def over_col(k):
        return (r, col_peer(k))

    wides = {1: (xa1, xb1, xc1, xd1), 3: (xa3, xb3, xc3, xd3)}

    def wide_start(value, tag):
        a, b = wides[tag][:2]
        a[...] = value.reshape(8, 16, B)

        def send(k):
            to = row_peer(k)
            remote(a.at[to], b.at[r], sa_s.at[tag], sa_r.at[tag], (to, c)).start()

        loop(1, 8, send)

    def wide_second(tag):
        a, b, d = wides[tag][:3]
        collect(b, 8, sa_s.at[tag], sa_r.at[tag])
        b[r] = a[r]
        d[c] = added(b, 8)
        spread(d, c, 16, sb_s.at[tag], sb_r.at[tag], over_col)

    def wide_third(tag):
        d, e = wides[tag][2:]
        collect(d, 16, sb_s.at[tag], sb_r.at[tag])
        e[r] = added(d, 16)
        spread(e, r, 8, sc_s.at[tag], sc_r.at[tag], over_row)

    def wide_end(tag):
        e = wides[tag][3]
        collect(e, 8, sc_s.at[tag], sc_r.at[tag])
        return e[...].reshape(B, B)

    turn_start(0, st)
    loop(1, 8, lambda k: ag1(k).start())
    turn_wait(0, st)
    gather_start(st, 0)
    def cat(i):
        high, rest = halves(vcol[:, block(i)].T)
        scat[block(i), :B] = high
        scat[block(i), B:] = rest

    cat(r)

    def ag1_wait(k):
        i = lax.rem(r + 8 - k, 8)
        remote(vcol.at[:, block(i)], vcol.at[:, block(i)], ag1_s.at[0], ag1_r.at[i], (r, c)).wait_recv()
        cat(i)

    loop(1, 8, ag1_wait)

    ga[c] = fine(vcol[pl.ds(pl.multiple_of(r * 16, 16), 16), :], vcol[...], NT)
    spread(ga, c, 16, sb_s.at[0], sb_r.at[0], over_col)

    def times(first, parity):
        a = chi[pl.ds(first, 4), parity].reshape(512, COLS)
        b = clo[pl.ds(first, 4), parity].reshape(512, COLS)
        full = jnp.dot(a, scat[...], preferred_element_type=F32) + jnp.dot(b, scat[...], preferred_element_type=F32)
        return (full[:, :B] + full[:, B:]).reshape(4, B, B)

    def across(h):
        return remote(ypart.at[pl.ds(h * 4, 4)], d2d.at[pl.ds(h * 4, 4)], d2d_s.at[h], d2d_r.at[h], (r, partner))

    def theirs(h):
        ypart[pl.ds(h * 4, 4)] = times(h * 4, 1 - core)
        across(h).start()

    loop(0, 2, theirs)

    def ours(h):
        yown[pl.ds(h * 4, 4)] = times(h * 4, core)

    loop(0, 2, ours)

    def rs2_copy(i):
        return remote(yown.at[i], rs2.at[chip], rs2_s.at[0], rs2_r.at[0], (r, 2 * i + core))

    def combine(h):
        across(h).wait_recv()
        for t in range(4):
            i = h * 4 + t
            yown[i] = yown[i] + d2d[i]

            @pl.when(i != chip)
            def _():
                rs2_copy(i).start()

    loop(0, 2, combine)

    gather_relay(st, 0)

    bent0 = fine(st[:, block(core)], yown[0])
    for i in range(1, 8):
        bent0 = bent0 + fine(st[:, block(2 * i + core)], yown[i])
    wide_start(bent0, 1)

    collect(ga, 16, sb_s.at[0], sb_r.at[0])
    gb[r] = added(ga, 16)
    spread(gb, r, 8, sc_s.at[0], sc_r.at[0], over_row)

    seven(yown, rs2, rs2_s, rs2_r).wait_recv()
    rs2[chip] = yown[chip]
    yt[:, block(c)] = added(rs2, 8).T
    wide_second(1)
    gather_start(yt, 1)

    collect(gb, 8, sc_s.at[0], sc_r.at[0])
    factor_start(gb[...].reshape(B, B), aug)
    factor_half(aug, low0, 0)
    factor_half(aug, low0, 1)
    wide_third(1)
    inv0 = low0[:, B:]

    gather_wait(st, 0)

    def put(i):
        return pltpu.make_async_copy(pt.at[pl.ds(i * B, B)], p_out.at[pl.ds(i * B, B)], osem.at[0])

    def first_q(i):
        o = pl.ds(i * 512, 512)
        pt[0:B, o] = fine(inv0, st[:, o])

    for i in range(4):
        first_q(i)

    put(0).start()
    gather_relay(yt, 1)
    gather_wait(yt, 1)

    def small_start(value, buf, tag):
        buf[r] = value
        spread(buf, r, 8, sa_s.at[tag], sa_r.at[tag], over_row)

    def small_middle(buf, out, tag):
        collect(buf, 8, sa_s.at[tag], sa_r.at[tag])
        out[c] = added(buf, 8)
        spread(out, c, 16, sb_s.at[tag], sb_r.at[tag], over_col)

    def small_end(out, n, tag):
        collect(out, 16, sb_s.at[tag], sb_r.at[tag])
        return out[...].reshape(16 * n, B)

    def share(n):
        return pl.ds(pl.multiple_of(c * n, 8), n)

    def first_image(i):
        o = pl.ds(i * 512, 512)
        pt[2 * B : 3 * B, o] = fine(inv0, yt[:, o])

    for i in range(4):
        first_image(i)

    first_pass[...] = jnp.zeros((3 * B, 2 * B), F32)
    projection[...] = jnp.zeros((3 * B, 2 * B), F32)
    h1 = exact(exact(inv0, wide_end(1)), inv0, NT)
    first_pass[0:B, 0:B] = h1
    h1t = h1.T

    def once(i):
        o = pl.ds(i * 512, 512)
        w = pt[2 * B : 3 * B, o] - fine(h1t, pt[0:B, o])
        pt[B : 2 * B, o] = w
        high, rest = halves(w)
        wt[0:B, o] = high
        wt[B : 2 * B, o] = rest

    for i in range(4):
        once(i)


    tsh[2] = pt[B : 2 * B, block(c)]

    @pl.when(jnp.logical_not(stays))
    def _():
        remote(tsh.at[2], tsh.at[3], t_s.at[2], t_r.at[2], origin).start()

    def times_t(k):
        q = lax.rem(lax.div(r, 2) + 1 + k, 4)
        o = pl.ds(pl.multiple_of(q * 256, 256), 256)
        a = chi[:, :, :, o].reshape(ROWS, 256)
        b = clo[:, :, :, o].reshape(ROWS, 256)
        full = jnp.dot(wt[...], a, preferred_element_type=F32)
        half = full[:B, :] + (full[B:, :] + jnp.dot(wt[0:B, :], b, preferred_element_type=F32))
        y1p[2 * q] = half[:, :B]
        y1p[2 * q + 1] = half[:, B:]
        for t in range(2):
            to = 2 * q + t

            @pl.when(to != r)
            def _():
                remote(y1p.at[to], rs3.at[r], rs3_s.at[0], rs3_r.at[0], (to, c)).start()

    loop(0, 4, times_t)

    small_start(fine(pt[share(24), :], pt[B : 2 * B, :], NT), ia, 2)
    fresh1 = row_sum(y1p, rs3, rs3_s, rs3_r)
    tsh[1] = fresh1
    turn_start(1, zt)

    @pl.when(jnp.logical_not(stays))
    def _():
        remote(tsh.at[2], tsh.at[3], t_s.at[2], t_r.at[2], origin).wait_recv()

    @pl.when(stays)
    def _():
        tsh[3] = tsh[2]

    wide_start(exact(tsh[3], tsh[1], NT), 3)
    small_middle(ia, ib, 2)
    wide_second(3)
    turn_wait(1, zt)
    gather_start(zt, 2)
    sums = small_end(ib, 24, 2)
    h2 = sums[0:B, :]
    h2t = h2.T
    crossed = sums[2 * B : 3 * B, :]
    projection[0:B, 0:B] = h1 + h2
    factor_start(sums[B : 2 * B, :] - exact(h2t, h2), aug)
    factor_half(aug, low1, 0)
    wide_third(3)
    factor_half(aug, low1, 1)
    projection[B : 2 * B, 0:B] = low1[:, :B]
    inv1 = low1[:, B:]
    tail = exact(inv1, h2t)
    mix1 = jnp.concatenate([-tail, inv1], axis=1)

    def second_q(i):
        o = pl.ds(i * 512, 512)
        pt[B : 2 * B, o] = fine(mix1, pt[0 : 2 * B, o])

    for i in range(4):
        second_q(i)

    put(1).start()

    top = exact(crossed - exact(h1t, h2), inv1, NT)
    bent = exact(h2t, crossed - exact(h1, h2) * 0.5)
    first_pass[0:B, B : 2 * B] = top
    gather_relay(zt, 2)
    below = exact(exact(inv1, wide_end(3) - bent - bent.T), inv1, NT)
    first_pass[B : 2 * B, B : 2 * B] = below
    passed = pltpu.make_async_copy(first_pass, f_out, osem.at[1])
    passed.start()
    mix[...] = jnp.concatenate([inv1, -top.T, -below.T, -tail], axis=1)
    gather_wait(zt, 2)

    def once1(i):
        o = pl.ds(i * 512, 512)
        pt[2 * B : 3 * B, o] = fine(mix[...], jnp.concatenate([zt[:, o], pt[:, o]], axis=0))

    for i in range(4):
        once1(i)

    put(2).start()
    small_start(fine(pt[share(24), :], pt[2 * B : 3 * B, :], NT), ka, 4)
    small_middle(ka, kb, 4)
    sums1 = small_end(kb, 24, 4)
    h2b = sums1[0 : 2 * B, :]
    projection[0:B, B : 2 * B] = top + h2b[0:B]
    projection[B : 2 * B, B : 2 * B] = below + h2b[B:]
    factor_start(sums1[2 * B : 3 * B, :] - exact(h2b, h2b, TN), aug)
    factor_half(aug, low2, 0)
    factor_half(aug, low2, 1)
    projection[2 * B : 3 * B, B : 2 * B] = low2[:, :B]
    inv2 = low2[:, B:]
    projected = pltpu.make_async_copy(projection, h_out, osem.at[2])
    projected.start()
    last[...] = jnp.concatenate([-exact(inv2, h2b, NT), inv2], axis=1)
    mixed = pltpu.make_async_copy(last, l_out, osem.at[3])
    mixed.start()

    seven(stp, rs1, rs1_s, rs1_r).wait_send()
    seven(yown, rs2, rs2_s, rs2_r).wait_send()
    seven(y1p, rs3, rs3_s, rs3_r).wait_send()
    ag1_sent().wait_send()

    @pl.when(jnp.logical_not(stays))
    def _():
        for tag in range(3):
            turn(tag, zt, c, there).wait_send()

    loop(0, 2, lambda h: across(h).wait_send())
    for tag, buf in enumerate((st, yt, zt)):
        gather_sent(buf, tag)
    rest(ga, 16, sb_s.at[0], sb_r.at[0]).wait_send()
    rest(gb, 8, sc_s.at[0], sc_r.at[0]).wait_send()
    for tag, (a, b) in ((2, (ia, ib)), (4, (ka, kb))):
        rest(a, 8, sa_s.at[tag], sa_r.at[tag]).wait_send()
        rest(b, 16, sb_s.at[tag], sb_r.at[tag]).wait_send()
    for tag in (1, 3):
        rest(wides[tag][0], 8, sa_s.at[tag], sa_r.at[tag]).wait_send()
        rest(wides[tag][2], 16, sb_s.at[tag], sb_r.at[tag]).wait_send()
        rest(wides[tag][3], 8, sc_s.at[tag], sc_r.at[tag]).wait_send()
    pltpu.make_async_copy(pt, p_out, osem.at[0]).wait()
    passed.wait()
    projected.wait()
    mixed.wait()


def finish(p, l, h, f, basis, projection, first_pass):
    basis[:, : 2 * B] = p[: 2 * B, :].T * F32(N**0.5)
    basis[:, 2 * B :] = fine(l[...], p[...]).T * F32(N**0.5)
    projection[...] = h[...]
    first_pass[...] = f[...]


def local(covariance, seed_index):
    v = pltpu.VMEM
    dma = pltpu.SemaphoreType.DMA
    blocks8 = v((8, B, B), F32)
    wide = v((B, ROWS), F32)
    square = v((B, 2 * B), F32)
    small = [v((16, 16, B), F32), v((8, 16, B), F32)]
    for n in (24, 24):
        small += [v((8, n, B), F32), v((16, n, B), F32)]
    thin8, thin16 = v((8, 16, B), F32), v((16, 16, B), F32)
    scratch = [
        v((ROWS, COLS), F32), v((8, 2, B, COLS), BF16), v((8, 2, B, COLS), BF16),
        blocks8, blocks8, v((B, COLS), F32), wide,
        blocks8, blocks8, blocks8, blocks8, wide,
        wide, v((3 * B, ROWS), F32), v((2 * B, ROWS), BF16), blocks8, blocks8, v((4, B, B), F32),
        v((B, 3 * B), F32), v((3 * B, 2 * B), F32), v((3 * B, 2 * B), F32),
        v((COLS, 2 * B), BF16), square, square, square, square, v((B, 4 * B), F32), *small,
        *(thin8, thin8, thin16, thin8) * 2,
        dma((1,)), dma((4,)), dma((1,)), dma((1,)), dma((1,)), dma((8,)), dma((3,)), dma((3,)),
        dma((2,)), dma((2,)), dma((1,)), dma((1,)), dma((3,)), dma((3, 8)), dma((3,)), dma((3,)), dma((1,)), dma((1,)),
        dma((5,)), dma((5,)), dma((5,)), dma((5,)), dma((5,)), dma((5,)),
    ]
    any_space = pl.BlockSpec(memory_space=pl.ANY)
    wide_p, mixed, square_h, square_f = pl.pallas_call(
        kernel,
        out_shape=(
            jax.ShapeDtypeStruct((3 * B, ROWS), F32),
            jax.ShapeDtypeStruct((B, 3 * B), F32),
            jax.ShapeDtypeStruct((3 * B, 2 * B), F32),
            jax.ShapeDtypeStruct((3 * B, 2 * B), F32),
        ),
        in_specs=[pl.BlockSpec(memory_space=pltpu.SMEM), any_space],
        out_specs=[any_space] * 4,
        scratch_shapes=scratch,
        compiler_params=pltpu.CompilerParams(collective_id=0, has_side_effects=True, vmem_limit_bytes=60 * 2**20),
        name="lanczos",
    )(seed_index, covariance)
    whole = pl.BlockSpec((3 * B, 2 * B), lambda i: (0, 0))
    return pl.pallas_call(
        finish,
        grid=(2,),
        out_shape=(
            jax.ShapeDtypeStruct((ROWS, 3 * B), F32),
            jax.ShapeDtypeStruct((3 * B, 2 * B), F32),
            jax.ShapeDtypeStruct((3 * B, 2 * B), F32),
        ),
        in_specs=[pl.BlockSpec((3 * B, ROWS // 2), lambda i: (0, i)), pl.BlockSpec((B, 3 * B), lambda i: (0, 0)), whole, whole],
        out_specs=(pl.BlockSpec((ROWS // 2, 3 * B), lambda i: (i, 0)), whole, whole),
        name="finish",
    )(wide_p, mixed, square_h, square_f)


def solution(mesh):
    return jax.shard_map(
        local,
        mesh=mesh,
        in_specs=(P("row", "col"), P()),
        out_specs=(P("row", None), P(), P()),
        check_vma=False,
    )
```

```python
import jax
import jax.numpy as jnp
from jax import lax
from jax.experimental import pallas as pl
from jax.experimental.pallas import tpu as pltpu
from jax.sharding import PartitionSpec as P

N = 16384
B = 128
ITERS = 2
ROWS = 2048
COLS = 1024
NB = 16
MESH = pl.DeviceIdType.MESH
F32 = jnp.float32
BF16 = jnp.bfloat16
NN = (((1,), (0,)), ((), ()))
NT = (((1,), (1,)), ((), ()))
TN = (((0,), (0,)), ((), ()))
FAR_FIRST = ((2, 1), (2, 0), (1, 1), (3, 1), (0, 1), (1, 0), (3, 0))


def halves(a):
    high = a.astype(BF16)
    return high, (a - high.astype(F32)).astype(BF16)


def exact(a, b, dims=NN):
    def thirds(x):
        high = x.astype(BF16)
        rest = x - high.astype(F32)
        middle = rest.astype(BF16)
        return high, middle, (rest - middle.astype(F32)).astype(BF16)

    (over_a,), (over_b,) = dims[0]
    ah, am, al = thirds(a)
    bh, bm, bl = thirds(b)
    left = jnp.concatenate([al, am, ah, am, ah, ah], axis=over_a)
    right = jnp.concatenate([bh, bm, bl, bh, bm, bh], axis=over_b)
    return lax.dot_general(left, right, dims, preferred_element_type=F32)


def fine(a, b, dims=NN):
    ah, al = halves(a)
    bh, bl = halves(b)

    def dot(x, y):
        return lax.dot_general(x, y, dims, preferred_element_type=F32)

    both = dot(jnp.concatenate([ah, al], axis=0), bh)
    n = a.shape[0]
    return both[:n] + (both[n:] + dot(ah, bl))


def factor_start(gram, aug):
    rows = lax.broadcasted_iota(jnp.int32, (B, B), 0)
    lanes = lax.broadcasted_iota(jnp.int32, (B, B), 1)
    aug[:, :B] = gram
    aug[:, B:] = jnp.where(rows == lanes, 1.0, 0.0).astype(F32)


def factor_half(aug, low, half):
    lane = lax.broadcasted_iota(jnp.int32, (NB, B), 1)
    sub = lax.broadcasted_iota(jnp.int32, (NB, B), 0)

    def panel(p, carry):
        o = pl.multiple_of(p * NB, NB)
        left = aug[pl.ds(o, NB), :B]
        right = aug[pl.ds(o, NB), B:]
        cols = []
        for t in range(NB):
            one = jnp.sum(jnp.where(lane == o + t, left, 0.0), axis=1, keepdims=True)
            cols.append(jnp.broadcast_to(one, (NB, B)))
        for t in range(NB):
            inv = lax.rsqrt(cols[t][t : t + 1, :])
            scale = jnp.where(sub == t, inv, 1.0)
            ratio = jnp.where(sub > t, cols[t] * inv, 0.0)
            left = left * scale
            right = right * scale
            left = left - ratio * left[t : t + 1, :]
            right = right - ratio * right[t : t + 1, :]
            for u in range(t + 1, NB):
                cols[u] = cols[u] - ratio * (cols[u][t : t + 1, :] * inv)
        left = jnp.where(lane >= o, left, 0.0)
        low[pl.ds(o, NB), :B] = jnp.where(lane >= o + sub, left, 0.0)
        low[pl.ds(o, NB), B:] = right
        both = jnp.concatenate([left, right], axis=1)
        aug[...] = aug[...] - exact(left, both, TN)
        return carry

    lax.fori_loop(half * (B // NB // 2), (half + 1) * (B // NB // 2), panel, 0)


def kernel(
    seed, cov, p_out, l_out, h_out, f_out,
    cvm, chi, clo, stp, rs1, vcol, st, ypart, d2d, yown, rs2, yt, zt, pt, wt, y1p, rs3, tsh, last, projection, first_pass,
    scat, aug, low0, low1, low2, mix, ga, gb, ia, ib, ka, kb, xa1, xb1, xc1, xd1, xa3, xb3, xc3, xd3,
    csem, osem, rs1_s, rs1_r, ag1_s, ag1_r, t_s, t_r, d2d_s, d2d_r, rs2_s, rs2_r, ag_s, ag_r, fw_s, fw_r, rs3_s, rs3_r,
    sa_s, sa_r, sb_s, sb_r, sc_s, sc_r,
):
    r = lax.axis_index("row")
    c = lax.axis_index("col")
    core = lax.rem(c, 2)
    chip = lax.div(c, 2)
    partner = c + 1 - 2 * core
    there = (chip, core * 8 + r)
    origin = (lax.rem(c, 8), 2 * r + lax.div(c, 8))
    stays = jnp.logical_and(there[0] == r, there[1] == c)

    def loop(lo, hi, body):
        def run(i, carry):
            body(i)
            return carry

        lax.fori_loop(lo, hi, run, 0)

    def remote(src, dst, ssem, rsem, dev):
        return pltpu.make_async_remote_copy(src, dst, ssem, rsem, device_id=dev, device_id_type=MESH)

    def row_peer(k):
        return lax.rem(r + k, 8)

    def row_at(d):
        return 2 * lax.rem(lax.div(r, 2) + d[0], 4) + lax.rem(lax.rem(r, 2) + d[1], 2)

    def chip_at(d):
        return 4 * lax.rem(lax.div(chip, 4) + d[1], 2) + lax.rem(lax.rem(chip, 4) + d[0], 4)

    def back(d):
        return ((4 - d[0]) % 4, d[1])

    def col_peer(k):
        return lax.rem(c + k, 16)

    def added(buf, n):
        total = buf[0]
        for i in range(1, n):
            total = total + buf[i]
        return total

    def block(i):
        return pl.ds(pl.multiple_of(i * B, B), B)

    def load(i):
        return pltpu.make_async_copy(cov.at[pl.ds(i * 256, 256)], cvm.at[pl.ds(i * 256, 256)], csem.at[0])

    loop(0, 8, lambda i: load(i).start())
    barrier = pltpu.get_barrier_semaphore()

    def greet(dev):
        pl.semaphore_signal(barrier, inc=1, device_id=dev, device_id_type=MESH)

    loop(1, 8, lambda k: greet((row_peer(k), c)))
    loop(1, 16, lambda k: greet((r, col_peer(k))))

    @pl.when(jnp.logical_not(stays))
    def _():
        greet(there)
        greet(origin)

    pltpu.make_async_copy(cov, cvm, csem.at[0]).wait()

    def gather(i):
        lines = []
        for t in range(8):
            at = seed[i * 8 + t] - r * ROWS
            inside = (at >= 0) & (at < ROWS)
            line = cvm[pl.ds(jnp.clip(at, 0, ROWS - 1), 1), :]
            lines.append(jnp.where(inside, line, 0.0))
        full = jnp.concatenate(lines, axis=0)
        for b in range(8):
            stp[b, pl.ds(pl.multiple_of(i * 8, 8), 8), :] = full[:, b * B : (b + 1) * B]

    loop(0, B // 8, gather)

    @pl.when(stays)
    def _():
        pl.semaphore_wait(barrier, 22)

    @pl.when(jnp.logical_not(stays))
    def _():
        pl.semaphore_wait(barrier, 24)

    def rs1_send(to):
        remote(stp.at[to], rs1.at[r], rs1_s.at[0], rs1_r.at[0], (to, c)).start()

    for d in FAR_FIRST:
        rs1_send(row_at(d))

    def split(i):
        high, rest = halves(cvm[block(i), :])
        chi[lax.div(i, 2), lax.rem(i, 2)] = high
        clo[lax.div(i, 2), lax.rem(i, 2)] = rest

    loop(0, 16, split)

    def seven(src, dst, ssem, rsem):
        return remote(src.at[pl.ds(0, 7)], dst.at[pl.ds(0, 7)], ssem.at[0], rsem.at[0], (r, c))

    def row_sum(src, dst, ssem, rsem):
        seven(src, dst, ssem, rsem).wait_recv()
        dst[r] = src[r]
        return added(dst, 8)

    start = row_sum(stp, rs1, rs1_s, rs1_r)
    vcol[:, block(r)] = start
    tsh[0] = start

    def ag1(to):
        return remote(vcol.at[:, block(r)], vcol.at[:, block(r)], ag1_s.at[0], ag1_r.at[r], (to, c))


    def turn(tag, dst, at, dev):
        return remote(tsh.at[tag], dst.at[0:B, block(at)], t_s.at[tag], t_r.at[tag], dev)

    def turn_start(tag, dst):
        @pl.when(jnp.logical_not(stays))
        def _():
            turn(tag, dst, there[1], there).start()

    def turn_wait(tag, dst):
        @pl.when(jnp.logical_not(stays))
        def _():
            turn(tag, dst, c, there).wait_recv()

        @pl.when(stays)
        def _():
            dst[0:B, block(c)] = tsh[tag]


    def ag1_sent():
        return remote(vcol.at[:, pl.ds(0, 7 * B)], vcol.at[:, pl.ds(0, 7 * B)], ag1_s.at[0], ag1_r.at[0], (r, c))

    def gather_start(buf, tag):
        mine = buf.at[0:B, block(c)]

        def send(i):
            remote(mine, mine, ag_s.at[tag], ag_r.at[tag, chip], (r, 2 * i + core)).start()

        for d in FAR_FIRST:
            send(chip_at(d))
        remote(mine, mine, fw_s.at[tag], fw_r.at[tag], (r, partner)).start()

    def gather_relay(buf, tag):
        def relay(i):
            got = buf.at[0:B, block(2 * i + core)]
            remote(got, got, ag_s.at[tag], ag_r.at[tag, i], (r, c)).wait_recv()
            remote(got, got, fw_s.at[tag], fw_r.at[tag], (r, partner)).start()

        for d in FAR_FIRST:
            relay(chip_at(back(d)))

    def gather_all(buf, n, ssem, rsem, tag):
        got = buf.at[0:B, pl.ds(0, n * B)]
        return remote(got, got, ssem.at[tag], rsem.at[tag], (r, c))

    def gather_wait(buf, tag):
        gather_all(buf, 8, fw_s, fw_r, tag).wait_recv()

    def gather_sent(buf, tag):
        gather_all(buf, 7, ag_s, fw_r, tag).wait_send()
        gather_all(buf, 8, fw_s, fw_r, tag).wait_send()

    def spread(out, at, n_peers, ssem, rsem, devices):
        for dev in devices():
            remote(out.at[at], out.at[at], ssem, rsem, dev).start()

    def rest(out, n_peers, ssem, rsem):
        got = out.at[pl.ds(0, n_peers - 1)]
        return remote(got, got, ssem, rsem, (r, c))

    def collect(out, n_peers, ssem, rsem):
        rest(out, n_peers, ssem, rsem).wait_recv()

    def over_row():
        return [(row_at(d), c) for d in FAR_FIRST]

    def over_col():
        far = [(r, 2 * chip_at(d) + o) for d in FAR_FIRST for o in (core, 1 - core)]
        return far + [(r, partner)]

    wides = {1: (xa1, xb1, xc1, xd1), 3: (xa3, xb3, xc3, xd3)}

    def wide_start(value, tag):
        a, b = wides[tag][:2]
        a[...] = value.reshape(8, 16, B)

        for d in FAR_FIRST:
            to = row_at(d)
            remote(a.at[to], b.at[r], sa_s.at[tag], sa_r.at[tag], (to, c)).start()


    def wide_second(tag):
        a, b, d = wides[tag][:3]
        collect(b, 8, sa_s.at[tag], sa_r.at[tag])
        b[r] = a[r]
        d[c] = added(b, 8)
        spread(d, c, 16, sb_s.at[tag], sb_r.at[tag], over_col)

    def wide_third(tag):
        d, e = wides[tag][2:]
        collect(d, 16, sb_s.at[tag], sb_r.at[tag])
        e[r] = added(d, 16)
        spread(e, r, 8, sc_s.at[tag], sc_r.at[tag], over_row)

    def wide_end(tag):
        e = wides[tag][3]
        collect(e, 8, sc_s.at[tag], sc_r.at[tag])
        return e[...].reshape(B, B)

    turn_start(0, st)
    for d in FAR_FIRST:
        ag1(row_at(d)).start()
    turn_wait(0, st)
    gather_start(st, 0)
    def cat(i):
        high, rest = halves(vcol[:, block(i)].T)
        scat[block(i), :B] = high
        scat[block(i), B:] = rest

    cat(r)

    def ag1_wait(i):
        remote(vcol.at[:, block(i)], vcol.at[:, block(i)], ag1_s.at[0], ag1_r.at[i], (r, c)).wait_recv()
        cat(i)

    for d in FAR_FIRST:
        ag1_wait(row_at(back(d)))


    ga[c] = fine(vcol[pl.ds(pl.multiple_of(r * 16, 16), 16), :], vcol[...], NT)
    spread(ga, c, 16, sb_s.at[0], sb_r.at[0], over_col)

    def times(first, parity):
        a = chi[pl.ds(first, 4), parity].reshape(512, COLS)
        b = clo[pl.ds(first, 4), parity].reshape(512, COLS)
        full = jnp.dot(a, scat[...], preferred_element_type=F32) + jnp.dot(b, scat[...], preferred_element_type=F32)
        return (full[:, :B] + full[:, B:]).reshape(4, B, B)

    def across(h):
        return remote(ypart.at[pl.ds(h * 4, 4)], d2d.at[pl.ds(h * 4, 4)], d2d_s.at[h], d2d_r.at[h], (r, partner))

    def half_at(n):
        return lax.rem(lax.div(chip, 4) + 1 + n, 2)

    def theirs(n):
        h = half_at(n)
        ypart[pl.ds(h * 4, 4)] = times(h * 4, 1 - core)
        across(h).start()

    loop(0, 2, theirs)

    def ours(n):
        h = half_at(n)
        yown[pl.ds(h * 4, 4)] = times(h * 4, core)

    loop(0, 2, ours)

    def rs2_copy(i):
        return remote(yown.at[i], rs2.at[chip], rs2_s.at[0], rs2_r.at[0], (r, 2 * i + core))

    def combine(n):
        h = half_at(n)
        across(h).wait_recv()
        for t in (2, 1, 3, 0):
            i = h * 4 + lax.rem(lax.rem(chip, 4) + t, 4)
            yown[i] = yown[i] + d2d[i]

            @pl.when(i != chip)
            def _():
                rs2_copy(i).start()

    loop(0, 2, combine)

    gather_relay(st, 0)

    bent0 = fine(st[:, block(core)], yown[0])
    for i in range(1, 8):
        bent0 = bent0 + fine(st[:, block(2 * i + core)], yown[i])
    wide_start(bent0, 1)

    collect(ga, 16, sb_s.at[0], sb_r.at[0])
    gb[r] = added(ga, 16)
    spread(gb, r, 8, sc_s.at[0], sc_r.at[0], over_row)

    seven(yown, rs2, rs2_s, rs2_r).wait_recv()
    rs2[chip] = yown[chip]
    yt[:, block(c)] = added(rs2, 8).T
    wide_second(1)
    gather_start(yt, 1)

    collect(gb, 8, sc_s.at[0], sc_r.at[0])
    factor_start(gb[...].reshape(B, B), aug)
    factor_half(aug, low0, 0)
    factor_half(aug, low0, 1)
    wide_third(1)
    inv0 = low0[:, B:]

    gather_wait(st, 0)

    def put(i):
        return pltpu.make_async_copy(pt.at[pl.ds(i * B, B)], p_out.at[pl.ds(i * B, B)], osem.at[0])

    def first_q(i):
        o = pl.ds(i * 512, 512)
        pt[0:B, o] = fine(inv0, st[:, o])

    for i in range(4):
        first_q(i)

    put(0).start()
    gather_relay(yt, 1)
    gather_wait(yt, 1)

    def small_start(value, buf, tag):
        buf[r] = value
        spread(buf, r, 8, sa_s.at[tag], sa_r.at[tag], over_row)

    def small_middle(buf, out, tag):
        collect(buf, 8, sa_s.at[tag], sa_r.at[tag])
        out[c] = added(buf, 8)
        spread(out, c, 16, sb_s.at[tag], sb_r.at[tag], over_col)

    def small_end(out, n, tag):
        collect(out, 16, sb_s.at[tag], sb_r.at[tag])
        return out[...].reshape(16 * n, B)

    def share(n):
        return pl.ds(pl.multiple_of(c * n, 8), n)

    def first_image(i):
        o = pl.ds(i * 512, 512)
        pt[2 * B : 3 * B, o] = fine(inv0, yt[:, o])

    for i in range(4):
        first_image(i)

    first_pass[...] = jnp.zeros((3 * B, 2 * B), F32)
    projection[...] = jnp.zeros((3 * B, 2 * B), F32)
    h1 = exact(exact(inv0, wide_end(1)), inv0, NT)
    first_pass[0:B, 0:B] = h1
    h1t = h1.T

    def once(i):
        o = pl.ds(i * 512, 512)
        w = pt[2 * B : 3 * B, o] - fine(h1t, pt[0:B, o])
        pt[B : 2 * B, o] = w
        high, rest = halves(w)
        wt[0:B, o] = high
        wt[B : 2 * B, o] = rest

    for i in range(4):
        once(i)


    tsh[2] = pt[B : 2 * B, block(c)]

    @pl.when(jnp.logical_not(stays))
    def _():
        remote(tsh.at[2], tsh.at[3], t_s.at[2], t_r.at[2], origin).start()

    def times_t(k):
        q = lax.rem(lax.div(r, 2) + jnp.where(k == 0, 2, jnp.where(k == 1, 1, jnp.where(k == 2, 3, 0))), 4)
        o = pl.ds(pl.multiple_of(q * 256, 256), 256)
        a = chi[:, :, :, o].reshape(ROWS, 256)
        b = clo[:, :, :, o].reshape(ROWS, 256)
        full = jnp.dot(wt[...], a, preferred_element_type=F32)
        half = full[:B, :] + (full[B:, :] + jnp.dot(wt[0:B, :], b, preferred_element_type=F32))
        y1p[2 * q] = half[:, :B]
        y1p[2 * q + 1] = half[:, B:]
        for t in (1, 0):
            to = 2 * q + lax.rem(lax.rem(r, 2) + t, 2)

            @pl.when(to != r)
            def _():
                remote(y1p.at[to], rs3.at[r], rs3_s.at[0], rs3_r.at[0], (to, c)).start()

    loop(0, 4, times_t)

    small_start(fine(pt[share(24), :], pt[B : 2 * B, :], NT), ia, 2)
    fresh1 = row_sum(y1p, rs3, rs3_s, rs3_r)
    tsh[1] = fresh1
    turn_start(1, zt)

    @pl.when(jnp.logical_not(stays))
    def _():
        remote(tsh.at[2], tsh.at[3], t_s.at[2], t_r.at[2], origin).wait_recv()

    @pl.when(stays)
    def _():
        tsh[3] = tsh[2]

    wide_start(exact(tsh[3], tsh[1], NT), 3)
    small_middle(ia, ib, 2)
    wide_second(3)
    turn_wait(1, zt)
    gather_start(zt, 2)
    sums = small_end(ib, 24, 2)
    h2 = sums[0:B, :]
    h2t = h2.T
    crossed = sums[2 * B : 3 * B, :]
    projection[0:B, 0:B] = h1 + h2
    factor_start(sums[B : 2 * B, :] - exact(h2t, h2), aug)
    factor_half(aug, low1, 0)
    wide_third(3)
    factor_half(aug, low1, 1)
    projection[B : 2 * B, 0:B] = low1[:, :B]
    inv1 = low1[:, B:]
    tail = exact(inv1, h2t)
    mix1 = jnp.concatenate([-tail, inv1], axis=1)

    def second_q(i):
        o = pl.ds(i * 512, 512)
        pt[B : 2 * B, o] = fine(mix1, pt[0 : 2 * B, o])

    for i in range(4):
        second_q(i)

    put(1).start()

    top = exact(crossed - exact(h1t, h2), inv1, NT)
    bent = exact(h2t, crossed - exact(h1, h2) * 0.5)
    first_pass[0:B, B : 2 * B] = top
    gather_relay(zt, 2)
    below = exact(exact(inv1, wide_end(3) - bent - bent.T), inv1, NT)
    first_pass[B : 2 * B, B : 2 * B] = below
    passed = pltpu.make_async_copy(first_pass, f_out, osem.at[1])
    passed.start()
    mix[...] = jnp.concatenate([inv1, -top.T, -below.T, -tail], axis=1)
    gather_wait(zt, 2)

    def once1(i):
        o = pl.ds(i * 512, 512)
        pt[2 * B : 3 * B, o] = fine(mix[...], jnp.concatenate([zt[:, o], pt[:, o]], axis=0))

    for i in range(4):
        once1(i)

    put(2).start()
    small_start(fine(pt[share(24), :], pt[2 * B : 3 * B, :], NT), ka, 4)
    small_middle(ka, kb, 4)
    sums1 = small_end(kb, 24, 4)
    h2b = sums1[0 : 2 * B, :]
    projection[0:B, B : 2 * B] = top + h2b[0:B]
    projection[B : 2 * B, B : 2 * B] = below + h2b[B:]
    factor_start(sums1[2 * B : 3 * B, :] - exact(h2b, h2b, TN), aug)
    factor_half(aug, low2, 0)
    factor_half(aug, low2, 1)
    projection[2 * B : 3 * B, B : 2 * B] = low2[:, :B]
    inv2 = low2[:, B:]
    projected = pltpu.make_async_copy(projection, h_out, osem.at[2])
    projected.start()
    last[...] = jnp.concatenate([-exact(inv2, h2b, NT), inv2], axis=1)
    mixed = pltpu.make_async_copy(last, l_out, osem.at[3])
    mixed.start()

    seven(stp, rs1, rs1_s, rs1_r).wait_send()
    seven(yown, rs2, rs2_s, rs2_r).wait_send()
    seven(y1p, rs3, rs3_s, rs3_r).wait_send()
    ag1_sent().wait_send()

    @pl.when(jnp.logical_not(stays))
    def _():
        for tag in range(3):
            turn(tag, zt, c, there).wait_send()

    loop(0, 2, lambda h: across(h).wait_send())
    for tag, buf in enumerate((st, yt, zt)):
        gather_sent(buf, tag)
    rest(ga, 16, sb_s.at[0], sb_r.at[0]).wait_send()
    rest(gb, 8, sc_s.at[0], sc_r.at[0]).wait_send()
    for tag, (a, b) in ((2, (ia, ib)), (4, (ka, kb))):
        rest(a, 8, sa_s.at[tag], sa_r.at[tag]).wait_send()
        rest(b, 16, sb_s.at[tag], sb_r.at[tag]).wait_send()
    for tag in (1, 3):
        rest(wides[tag][0], 8, sa_s.at[tag], sa_r.at[tag]).wait_send()
        rest(wides[tag][2], 16, sb_s.at[tag], sb_r.at[tag]).wait_send()
        rest(wides[tag][3], 8, sc_s.at[tag], sc_r.at[tag]).wait_send()
    pltpu.make_async_copy(pt, p_out, osem.at[0]).wait()
    passed.wait()
    projected.wait()
    mixed.wait()


def finish(p, l, h, f, basis, projection, first_pass):
    basis[:, : 2 * B] = p[: 2 * B, :].T * F32(N**0.5)
    basis[:, 2 * B :] = fine(l[...], p[...]).T * F32(N**0.5)
    projection[...] = h[...]
    first_pass[...] = f[...]


def local(covariance, seed_index):
    v = pltpu.VMEM
    dma = pltpu.SemaphoreType.DMA
    blocks8 = v((8, B, B), F32)
    wide = v((B, ROWS), F32)
    square = v((B, 2 * B), F32)
    small = [v((16, 16, B), F32), v((8, 16, B), F32)]
    for n in (24, 24):
        small += [v((8, n, B), F32), v((16, n, B), F32)]
    thin8, thin16 = v((8, 16, B), F32), v((16, 16, B), F32)
    scratch = [
        v((ROWS, COLS), F32), v((8, 2, B, COLS), BF16), v((8, 2, B, COLS), BF16),
        blocks8, blocks8, v((B, COLS), F32), wide,
        blocks8, blocks8, blocks8, blocks8, wide,
        wide, v((3 * B, ROWS), F32), v((2 * B, ROWS), BF16), blocks8, blocks8, v((4, B, B), F32),
        v((B, 3 * B), F32), v((3 * B, 2 * B), F32), v((3 * B, 2 * B), F32),
        v((COLS, 2 * B), BF16), square, square, square, square, v((B, 4 * B), F32), *small,
        *(thin8, thin8, thin16, thin8) * 2,
        dma((1,)), dma((4,)), dma((1,)), dma((1,)), dma((1,)), dma((8,)), dma((3,)), dma((3,)),
        dma((2,)), dma((2,)), dma((1,)), dma((1,)), dma((3,)), dma((3, 8)), dma((3,)), dma((3,)), dma((1,)), dma((1,)),
        dma((5,)), dma((5,)), dma((5,)), dma((5,)), dma((5,)), dma((5,)),
    ]
    any_space = pl.BlockSpec(memory_space=pl.ANY)
    wide_p, mixed, square_h, square_f = pl.pallas_call(
        kernel,
        out_shape=(
            jax.ShapeDtypeStruct((3 * B, ROWS), F32),
            jax.ShapeDtypeStruct((B, 3 * B), F32),
            jax.ShapeDtypeStruct((3 * B, 2 * B), F32),
            jax.ShapeDtypeStruct((3 * B, 2 * B), F32),
        ),
        in_specs=[pl.BlockSpec(memory_space=pltpu.SMEM), any_space],
        out_specs=[any_space] * 4,
        scratch_shapes=scratch,
        compiler_params=pltpu.CompilerParams(collective_id=0, has_side_effects=True, vmem_limit_bytes=60 * 2**20),
        name="lanczos",
    )(seed_index, covariance)
    whole = pl.BlockSpec((3 * B, 2 * B), lambda i: (0, 0))
    return pl.pallas_call(
        finish,
        grid=(2,),
        out_shape=(
            jax.ShapeDtypeStruct((ROWS, 3 * B), F32),
            jax.ShapeDtypeStruct((3 * B, 2 * B), F32),
            jax.ShapeDtypeStruct((3 * B, 2 * B), F32),
        ),
        in_specs=[pl.BlockSpec((3 * B, ROWS // 2), lambda i: (0, i)), pl.BlockSpec((B, 3 * B), lambda i: (0, 0)), whole, whole],
        out_specs=(pl.BlockSpec((ROWS // 2, 3 * B), lambda i: (i, 0)), whole, whole),
        name="finish",
    )(wide_p, mixed, square_h, square_f)


def solution(mesh):
    return jax.shard_map(
        local,
        mesh=mesh,
        in_specs=(P("row", "col"), P()),
        out_specs=(P("row", None), P(), P()),
        check_vma=False,
    )
```

```python
import jax
import jax.numpy as jnp
from jax import lax
from jax.experimental import pallas as pl
from jax.experimental.pallas import tpu as pltpu
from jax.sharding import PartitionSpec as P

N = 16384
B = 128
ITERS = 2
ROWS = 2048
COLS = 1024
NB = 16
MESH = pl.DeviceIdType.MESH
F32 = jnp.float32
BF16 = jnp.bfloat16
NN = (((1,), (0,)), ((), ()))
NT = (((1,), (1,)), ((), ()))
TN = (((0,), (0,)), ((), ()))
FAR_FIRST = ((2, 1), (2, 0), (1, 1), (3, 1), (0, 1), (1, 0), (3, 0))


def halves(a):
    high = a.astype(BF16)
    return high, (a - high.astype(F32)).astype(BF16)


def exact(a, b, dims=NN):
    def thirds(x):
        high = x.astype(BF16)
        rest = x - high.astype(F32)
        middle = rest.astype(BF16)
        return high, middle, (rest - middle.astype(F32)).astype(BF16)

    (over_a,), (over_b,) = dims[0]
    ah, am, al = thirds(a)
    bh, bm, bl = thirds(b)
    left = jnp.concatenate([al, am, ah, am, ah, ah], axis=over_a)
    right = jnp.concatenate([bh, bm, bl, bh, bm, bh], axis=over_b)
    return lax.dot_general(left, right, dims, preferred_element_type=F32)


def fine(a, b, dims=NN):
    ah, al = halves(a)
    bh, bl = halves(b)

    def dot(x, y):
        return lax.dot_general(x, y, dims, preferred_element_type=F32)

    both = dot(jnp.concatenate([ah, al], axis=0), bh)
    n = a.shape[0]
    return both[:n] + (both[n:] + dot(ah, bl))


def factor_start(gram, aug):
    rows = lax.broadcasted_iota(jnp.int32, (B, B), 0)
    lanes = lax.broadcasted_iota(jnp.int32, (B, B), 1)
    aug[:, :B] = gram
    aug[:, B:] = jnp.where(rows == lanes, 1.0, 0.0).astype(F32)


def factor_half(aug, low, half):
    lane = lax.broadcasted_iota(jnp.int32, (NB, B), 1)
    sub = lax.broadcasted_iota(jnp.int32, (NB, B), 0)

    def panel(p, carry):
        o = pl.multiple_of(p * NB, NB)
        left = aug[pl.ds(o, NB), :B]
        right = aug[pl.ds(o, NB), B:]
        cols = []
        for t in range(NB):
            one = jnp.sum(jnp.where(lane == o + t, left, 0.0), axis=1, keepdims=True)
            cols.append(jnp.broadcast_to(one, (NB, B)))
        for t in range(NB):
            inv = lax.rsqrt(cols[t][t : t + 1, :])
            scale = jnp.where(sub == t, inv, 1.0)
            ratio = jnp.where(sub > t, cols[t] * inv, 0.0)
            left = left * scale
            right = right * scale
            left = left - ratio * left[t : t + 1, :]
            right = right - ratio * right[t : t + 1, :]
            for u in range(t + 1, NB):
                cols[u] = cols[u] - ratio * (cols[u][t : t + 1, :] * inv)
        left = jnp.where(lane >= o, left, 0.0)
        low[pl.ds(o, NB), :B] = jnp.where(lane >= o + sub, left, 0.0)
        low[pl.ds(o, NB), B:] = right
        both = jnp.concatenate([left, right], axis=1)
        aug[...] = aug[...] - exact(left, both, TN)
        return carry

    lax.fori_loop(half * (B // NB // 2), (half + 1) * (B // NB // 2), panel, 0)


def kernel(
    seed, cov, p_out, l_out, h_out, f_out,
    cvm, chi, clo, stp, rs1, vcol, st, ypart, d2d, yown, rs2, yt, zt, pt, wt, y1p, rs3, tsh, last, projection, first_pass,
    scat, aug, low0, low1, low2, mix, ga, gb, ia, ib, ka, kb, xa1, xb1, xc1, xd1, xa3, xb3, xc3, xd3,
    csem, osem, rs1_s, rs1_r, ag1_s, ag1_r, t_s, t_r, d2d_s, d2d_r, rs2_s, rs2_r, ag_s, ag_r, fw_s, fw_r, rs3_s, rs3_r,
    sa_s, sa_r, sb_s, sb_r, sc_s, sc_r,
):
    r = lax.axis_index("row")
    c = lax.axis_index("col")
    core = lax.rem(c, 2)
    chip = lax.div(c, 2)
    partner = c + 1 - 2 * core
    there = (chip, core * 8 + r)
    origin = (lax.rem(c, 8), 2 * r + lax.div(c, 8))
    stays = jnp.logical_and(there[0] == r, there[1] == c)

    def loop(lo, hi, body):
        def run(i, carry):
            body(i)
            return carry

        lax.fori_loop(lo, hi, run, 0)

    def remote(src, dst, ssem, rsem, dev):
        return pltpu.make_async_remote_copy(src, dst, ssem, rsem, device_id=dev, device_id_type=MESH)

    def row_peer(k):
        return lax.rem(r + k, 8)

    def row_at(d):
        return 2 * lax.rem(lax.div(r, 2) + d[0], 4) + lax.rem(lax.rem(r, 2) + d[1], 2)

    def chip_at(d):
        return 4 * lax.rem(lax.div(chip, 4) + d[1], 2) + lax.rem(lax.rem(chip, 4) + d[0], 4)

    def back(d):
        return ((4 - d[0]) % 4, d[1])

    def col_peer(k):
        return lax.rem(c + k, 16)

    def added(buf, n):
        total = buf[0]
        for i in range(1, n):
            total = total + buf[i]
        return total

    def block(i):
        return pl.ds(pl.multiple_of(i * B, B), B)

    def load(i):
        return pltpu.make_async_copy(cov.at[pl.ds(i * 256, 256)], cvm.at[pl.ds(i * 256, 256)], csem.at[0])

    loop(0, 8, lambda i: load(i).start())
    barrier = pltpu.get_barrier_semaphore()

    def greet(dev):
        pl.semaphore_signal(barrier, inc=1, device_id=dev, device_id_type=MESH)

    loop(1, 8, lambda k: greet((row_peer(k), c)))
    loop(1, 16, lambda k: greet((r, col_peer(k))))

    @pl.when(jnp.logical_not(stays))
    def _():
        greet(there)
        greet(origin)

    pltpu.make_async_copy(cov, cvm, csem.at[0]).wait()

    def gather(i):
        lines = []
        for t in range(8):
            at = seed[i * 8 + t] - r * ROWS
            inside = (at >= 0) & (at < ROWS)
            line = cvm[pl.ds(jnp.clip(at, 0, ROWS - 1), 1), :]
            lines.append(jnp.where(inside, line, 0.0))
        full = jnp.concatenate(lines, axis=0)
        for b in range(8):
            stp[b, pl.ds(pl.multiple_of(i * 8, 8), 8), :] = full[:, b * B : (b + 1) * B]

    loop(0, B // 8, gather)

    @pl.when(stays)
    def _():
        pl.semaphore_wait(barrier, 22)

    @pl.when(jnp.logical_not(stays))
    def _():
        pl.semaphore_wait(barrier, 24)

    def rs1_send(to):
        remote(stp.at[to], rs1.at[r], rs1_s.at[0], rs1_r.at[0], (to, c)).start()

    for d in FAR_FIRST:
        rs1_send(row_at(d))

    def split(i):
        high, rest = halves(cvm[block(i), :])
        chi[lax.div(i, 2), lax.rem(i, 2)] = high
        clo[lax.div(i, 2), lax.rem(i, 2)] = rest

    loop(0, 16, split)

    def seven(src, dst, ssem, rsem):
        return remote(src.at[pl.ds(0, 7)], dst.at[pl.ds(0, 7)], ssem.at[0], rsem.at[0], (r, c))

    def row_sum(src, dst, ssem, rsem):
        seven(src, dst, ssem, rsem).wait_recv()
        dst[r] = src[r]
        return added(dst, 8)

    start = row_sum(stp, rs1, rs1_s, rs1_r)
    vcol[:, block(r)] = start
    tsh[0] = start

    def ag1(to):
        return remote(vcol.at[:, block(r)], vcol.at[:, block(r)], ag1_s.at[0], ag1_r.at[r], (to, c))


    def turn(tag, dst, at, dev):
        return remote(tsh.at[tag], dst.at[0:B, block(at)], t_s.at[tag], t_r.at[tag], dev)

    def turn_start(tag, dst):
        @pl.when(jnp.logical_not(stays))
        def _():
            turn(tag, dst, there[1], there).start()

    def turn_wait(tag, dst):
        @pl.when(jnp.logical_not(stays))
        def _():
            turn(tag, dst, c, there).wait_recv()

        @pl.when(stays)
        def _():
            dst[0:B, block(c)] = tsh[tag]


    def ag1_sent():
        return remote(vcol.at[:, pl.ds(0, 7 * B)], vcol.at[:, pl.ds(0, 7 * B)], ag1_s.at[0], ag1_r.at[0], (r, c))

    def gather_start(buf, tag):
        mine = buf.at[0:B, block(c)]

        def send(i):
            remote(mine, mine, ag_s.at[tag], ag_r.at[tag, chip], (r, 2 * i + core)).start()

        for d in FAR_FIRST:
            send(chip_at(d))
        remote(mine, mine, fw_s.at[tag], fw_r.at[tag], (r, partner)).start()

    def gather_relay(buf, tag):
        def relay(i):
            got = buf.at[0:B, block(2 * i + core)]
            remote(got, got, ag_s.at[tag], ag_r.at[tag, i], (r, c)).wait_recv()
            remote(got, got, fw_s.at[tag], fw_r.at[tag], (r, partner)).start()

        for d in FAR_FIRST:
            relay(chip_at(back(d)))

    def gather_all(buf, n, ssem, rsem, tag):
        got = buf.at[0:B, pl.ds(0, n * B)]
        return remote(got, got, ssem.at[tag], rsem.at[tag], (r, c))

    def gather_wait(buf, tag):
        gather_all(buf, 8, fw_s, fw_r, tag).wait_recv()

    def gather_sent(buf, tag):
        gather_all(buf, 7, ag_s, fw_r, tag).wait_send()
        gather_all(buf, 8, fw_s, fw_r, tag).wait_send()

    def spread(out, at, n_peers, ssem, rsem, devices):
        for dev in devices():
            remote(out.at[at], out.at[at], ssem, rsem, dev).start()

    def rest(out, n_peers, ssem, rsem):
        got = out.at[pl.ds(0, n_peers - 1)]
        return remote(got, got, ssem, rsem, (r, c))

    def collect(out, n_peers, ssem, rsem):
        rest(out, n_peers, ssem, rsem).wait_recv()

    def over_row():
        return [(row_at(d), c) for d in FAR_FIRST]

    def over_col():
        far = [(r, 2 * chip_at(d) + o) for d in FAR_FIRST for o in (core, 1 - core)]
        return far + [(r, partner)]

    wides = {1: (xa1, xb1, xc1, xd1), 3: (xa3, xb3, xc3, xd3)}

    def wide_start(value, tag):
        a, b = wides[tag][:2]
        a[...] = value.reshape(8, 16, B)

        for d in FAR_FIRST:
            to = row_at(d)
            remote(a.at[to], b.at[r], sa_s.at[tag], sa_r.at[tag], (to, c)).start()


    def wide_second(tag):
        a, b, d = wides[tag][:3]
        collect(b, 8, sa_s.at[tag], sa_r.at[tag])
        b[r] = a[r]
        d[c] = added(b, 8)
        spread(d, c, 16, sb_s.at[tag], sb_r.at[tag], over_col)

    def wide_third(tag):
        d, e = wides[tag][2:]
        collect(d, 16, sb_s.at[tag], sb_r.at[tag])
        e[r] = added(d, 16)
        spread(e, r, 8, sc_s.at[tag], sc_r.at[tag], over_row)

    def wide_end(tag):
        e = wides[tag][3]
        collect(e, 8, sc_s.at[tag], sc_r.at[tag])
        return e[...].reshape(B, B)

    turn_start(0, st)
    for d in FAR_FIRST:
        ag1(row_at(d)).start()
    turn_wait(0, st)
    gather_start(st, 0)
    def cat(i):
        high, rest = halves(vcol[:, block(i)].T)
        scat[block(i), :B] = high
        scat[block(i), B:] = rest

    cat(r)

    def ag1_wait(i):
        remote(vcol.at[:, block(i)], vcol.at[:, block(i)], ag1_s.at[0], ag1_r.at[i], (r, c)).wait_recv()
        cat(i)

    for d in FAR_FIRST:
        ag1_wait(row_at(back(d)))


    ga[c] = fine(vcol[pl.ds(pl.multiple_of(r * 16, 16), 16), :], vcol[...], NT)
    spread(ga, c, 16, sb_s.at[0], sb_r.at[0], over_col)

    def times(first, parity):
        a = chi[pl.ds(first, 4), parity].reshape(512, COLS)
        b = clo[pl.ds(first, 4), parity].reshape(512, COLS)
        full = jnp.dot(a, scat[...], preferred_element_type=F32) + jnp.dot(b, scat[...], preferred_element_type=F32)
        return (full[:, :B] + full[:, B:]).reshape(4, B, B)

    def across(h):
        return remote(ypart.at[pl.ds(h * 4, 4)], d2d.at[pl.ds(h * 4, 4)], d2d_s.at[h], d2d_r.at[h], (r, partner))

    def half_at(n):
        return lax.rem(lax.div(chip, 4) + 1 + n, 2)

    def theirs(n):
        h = half_at(n)
        ypart[pl.ds(h * 4, 4)] = times(h * 4, 1 - core)
        across(h).start()

    loop(0, 2, theirs)

    def ours(n):
        h = half_at(n)
        yown[pl.ds(h * 4, 4)] = times(h * 4, core)

    loop(0, 2, ours)

    def rs2_copy(i):
        return remote(yown.at[i], rs2.at[chip], rs2_s.at[0], rs2_r.at[0], (r, 2 * i + core))

    def combine(n):
        h = half_at(n)
        across(h).wait_recv()
        for t in (2, 1, 3, 0):
            i = h * 4 + lax.rem(lax.rem(chip, 4) + t, 4)
            yown[i] = yown[i] + d2d[i]

            @pl.when(i != chip)
            def _():
                rs2_copy(i).start()

    loop(0, 2, combine)

    gather_relay(st, 0)

    bent0 = fine(st[:, block(core)], yown[0])
    for i in range(1, 8):
        bent0 = bent0 + fine(st[:, block(2 * i + core)], yown[i])
    wide_start(bent0, 1)

    collect(ga, 16, sb_s.at[0], sb_r.at[0])
    gb[r] = added(ga, 16)
    spread(gb, r, 8, sc_s.at[0], sc_r.at[0], over_row)

    seven(yown, rs2, rs2_s, rs2_r).wait_recv()
    rs2[chip] = yown[chip]
    yt[:, block(c)] = added(rs2, 8).T
    wide_second(1)
    gather_start(yt, 1)

    collect(gb, 8, sc_s.at[0], sc_r.at[0])
    factor_start(gb[...].reshape(B, B), aug)
    factor_half(aug, low0, 0)
    factor_half(aug, low0, 1)
    wide_third(1)
    inv0 = low0[:, B:]

    gather_wait(st, 0)

    def put(i):
        return pltpu.make_async_copy(pt.at[pl.ds(i * B, B)], p_out.at[pl.ds(i * B, B)], osem.at[0])

    def first_q(i):
        o = pl.ds(i * 512, 512)
        pt[0:B, o] = fine(inv0, st[:, o])

    for i in range(4):
        first_q(i)

    put(0).start()
    gather_relay(yt, 1)
    gather_wait(yt, 1)

    def small_start(value, buf, tag):
        buf[r] = value
        spread(buf, r, 8, sa_s.at[tag], sa_r.at[tag], over_row)

    def small_middle(buf, out, tag):
        collect(buf, 8, sa_s.at[tag], sa_r.at[tag])
        out[c] = added(buf, 8)
        spread(out, c, 16, sb_s.at[tag], sb_r.at[tag], over_col)

    def small_end(out, n, tag):
        collect(out, 16, sb_s.at[tag], sb_r.at[tag])
        return out[...].reshape(16 * n, B)

    def share(n):
        return pl.ds(pl.multiple_of(c * n, 8), n)

    def first_image(i):
        o = pl.ds(i * 512, 512)
        pt[2 * B : 3 * B, o] = fine(inv0, yt[:, o])

    for i in range(4):
        first_image(i)

    first_pass[...] = jnp.zeros((3 * B, 2 * B), F32)
    projection[...] = jnp.zeros((3 * B, 2 * B), F32)
    h1 = exact(exact(inv0, wide_end(1)), inv0, NT)
    first_pass[0:B, 0:B] = h1
    h1t = h1.T

    def once(i):
        o = pl.ds(i * 512, 512)
        w = pt[2 * B : 3 * B, o] - fine(h1t, pt[0:B, o])
        pt[B : 2 * B, o] = w
        high, rest = halves(w)
        wt[0:B, o] = high
        wt[B : 2 * B, o] = rest

    for i in range(4):
        once(i)


    tsh[2] = pt[B : 2 * B, block(c)]

    @pl.when(jnp.logical_not(stays))
    def _():
        remote(tsh.at[2], tsh.at[3], t_s.at[2], t_r.at[2], origin).start()

    def times_t(k):
        q = lax.rem(lax.div(r, 2) + jnp.where(k == 0, 2, jnp.where(k == 1, 1, jnp.where(k == 2, 3, 0))), 4)
        o = pl.ds(pl.multiple_of(q * 256, 256), 256)
        a = chi[:, :, :, o].reshape(ROWS, 256)
        b = clo[:, :, :, o].reshape(ROWS, 256)
        full = jnp.dot(wt[...], a, preferred_element_type=F32)
        half = full[:B, :] + (full[B:, :] + jnp.dot(wt[0:B, :], b, preferred_element_type=F32))
        y1p[2 * q] = half[:, :B]
        y1p[2 * q + 1] = half[:, B:]
        for t in (1, 0):
            to = 2 * q + lax.rem(lax.rem(r, 2) + t, 2)

            @pl.when(to != r)
            def _():
                remote(y1p.at[to], rs3.at[r], rs3_s.at[0], rs3_r.at[0], (to, c)).start()

    loop(0, 4, times_t)

    small_start(fine(pt[share(24), :], pt[B : 2 * B, :], NT), ia, 2)
    fresh1 = row_sum(y1p, rs3, rs3_s, rs3_r)
    tsh[1] = fresh1
    turn_start(1, zt)

    @pl.when(jnp.logical_not(stays))
    def _():
        remote(tsh.at[2], tsh.at[3], t_s.at[2], t_r.at[2], origin).wait_recv()

    @pl.when(stays)
    def _():
        tsh[3] = tsh[2]

    wide_start(exact(tsh[3], tsh[1], NT), 3)
    small_middle(ia, ib, 2)
    wide_second(3)
    turn_wait(1, zt)
    gather_start(zt, 2)
    sums = small_end(ib, 24, 2)
    h2 = sums[0:B, :]
    h2t = h2.T
    crossed = sums[2 * B : 3 * B, :]
    projection[0:B, 0:B] = h1 + h2
    factor_start(sums[B : 2 * B, :] - exact(h2t, h2), aug)
    factor_half(aug, low1, 0)
    factor_half(aug, low1, 1)
    wide_third(3)
    projection[B : 2 * B, 0:B] = low1[:, :B]
    inv1 = low1[:, B:]
    tail = exact(inv1, h2t)
    mix1 = jnp.concatenate([-tail, inv1], axis=1)

    def second_q(i):
        o = pl.ds(i * 512, 512)
        pt[B : 2 * B, o] = fine(mix1, pt[0 : 2 * B, o])

    for i in range(4):
        second_q(i)

    put(1).start()

    top = exact(crossed - exact(h1t, h2), inv1, NT)
    bent = exact(h2t, crossed - exact(h1, h2) * 0.5)
    first_pass[0:B, B : 2 * B] = top
    gather_relay(zt, 2)
    below = exact(exact(inv1, wide_end(3) - bent - bent.T), inv1, NT)
    first_pass[B : 2 * B, B : 2 * B] = below
    passed = pltpu.make_async_copy(first_pass, f_out, osem.at[1])
    passed.start()
    mix[...] = jnp.concatenate([inv1, -top.T, -below.T, -tail], axis=1)
    gather_wait(zt, 2)

    def once1(i):
        o = pl.ds(i * 512, 512)
        pt[2 * B : 3 * B, o] = fine(mix[...], jnp.concatenate([zt[:, o], pt[:, o]], axis=0))

    for i in range(4):
        once1(i)

    put(2).start()
    small_start(fine(pt[share(24), :], pt[2 * B : 3 * B, :], NT), ka, 4)
    small_middle(ka, kb, 4)
    sums1 = small_end(kb, 24, 4)
    h2b = sums1[0 : 2 * B, :]
    projection[0:B, B : 2 * B] = top + h2b[0:B]
    projection[B : 2 * B, B : 2 * B] = below + h2b[B:]
    factor_start(sums1[2 * B : 3 * B, :] - exact(h2b, h2b, TN), aug)
    factor_half(aug, low2, 0)
    factor_half(aug, low2, 1)
    projection[2 * B : 3 * B, B : 2 * B] = low2[:, :B]
    inv2 = low2[:, B:]
    projected = pltpu.make_async_copy(projection, h_out, osem.at[2])
    projected.start()
    last[...] = jnp.concatenate([-exact(inv2, h2b, NT), inv2], axis=1)
    mixed = pltpu.make_async_copy(last, l_out, osem.at[3])
    mixed.start()

    seven(stp, rs1, rs1_s, rs1_r).wait_send()
    seven(yown, rs2, rs2_s, rs2_r).wait_send()
    seven(y1p, rs3, rs3_s, rs3_r).wait_send()
    ag1_sent().wait_send()

    @pl.when(jnp.logical_not(stays))
    def _():
        for tag in range(3):
            turn(tag, zt, c, there).wait_send()

    loop(0, 2, lambda h: across(h).wait_send())
    for tag, buf in enumerate((st, yt, zt)):
        gather_sent(buf, tag)
    rest(ga, 16, sb_s.at[0], sb_r.at[0]).wait_send()
    rest(gb, 8, sc_s.at[0], sc_r.at[0]).wait_send()
    for tag, (a, b) in ((2, (ia, ib)), (4, (ka, kb))):
        rest(a, 8, sa_s.at[tag], sa_r.at[tag]).wait_send()
        rest(b, 16, sb_s.at[tag], sb_r.at[tag]).wait_send()
    for tag in (1, 3):
        rest(wides[tag][0], 8, sa_s.at[tag], sa_r.at[tag]).wait_send()
        rest(wides[tag][2], 16, sb_s.at[tag], sb_r.at[tag]).wait_send()
        rest(wides[tag][3], 8, sc_s.at[tag], sc_r.at[tag]).wait_send()
    pltpu.make_async_copy(pt, p_out, osem.at[0]).wait()
    passed.wait()
    projected.wait()
    mixed.wait()


def finish(p, l, h, f, basis, projection, first_pass):
    basis[:, : 2 * B] = p[: 2 * B, :].T * F32(N**0.5)
    basis[:, 2 * B :] = fine(l[...], p[...]).T * F32(N**0.5)
    projection[...] = h[...]
    first_pass[...] = f[...]


def local(covariance, seed_index):
    v = pltpu.VMEM
    dma = pltpu.SemaphoreType.DMA
    blocks8 = v((8, B, B), F32)
    wide = v((B, ROWS), F32)
    square = v((B, 2 * B), F32)
    small = [v((16, 16, B), F32), v((8, 16, B), F32)]
    for n in (24, 24):
        small += [v((8, n, B), F32), v((16, n, B), F32)]
    thin8, thin16 = v((8, 16, B), F32), v((16, 16, B), F32)
    scratch = [
        v((ROWS, COLS), F32), v((8, 2, B, COLS), BF16), v((8, 2, B, COLS), BF16),
        blocks8, blocks8, v((B, COLS), F32), wide,
        blocks8, blocks8, blocks8, blocks8, wide,
        wide, v((3 * B, ROWS), F32), v((2 * B, ROWS), BF16), blocks8, blocks8, v((4, B, B), F32),
        v((B, 3 * B), F32), v((3 * B, 2 * B), F32), v((3 * B, 2 * B), F32),
        v((COLS, 2 * B), BF16), square, square, square, square, v((B, 4 * B), F32), *small,
        *(thin8, thin8, thin16, thin8) * 2,
        dma((1,)), dma((4,)), dma((1,)), dma((1,)), dma((1,)), dma((8,)), dma((3,)), dma((3,)),
        dma((2,)), dma((2,)), dma((1,)), dma((1,)), dma((3,)), dma((3, 8)), dma((3,)), dma((3,)), dma((1,)), dma((1,)),
        dma((5,)), dma((5,)), dma((5,)), dma((5,)), dma((5,)), dma((5,)),
    ]
    any_space = pl.BlockSpec(memory_space=pl.ANY)
    wide_p, mixed, square_h, square_f = pl.pallas_call(
        kernel,
        out_shape=(
            jax.ShapeDtypeStruct((3 * B, ROWS), F32),
            jax.ShapeDtypeStruct((B, 3 * B), F32),
            jax.ShapeDtypeStruct((3 * B, 2 * B), F32),
            jax.ShapeDtypeStruct((3 * B, 2 * B), F32),
        ),
        in_specs=[pl.BlockSpec(memory_space=pltpu.SMEM), any_space],
        out_specs=[any_space] * 4,
        scratch_shapes=scratch,
        compiler_params=pltpu.CompilerParams(collective_id=0, has_side_effects=True, vmem_limit_bytes=60 * 2**20),
        name="lanczos",
    )(seed_index, covariance)
    whole = pl.BlockSpec((3 * B, 2 * B), lambda i: (0, 0))
    return pl.pallas_call(
        finish,
        grid=(2,),
        out_shape=(
            jax.ShapeDtypeStruct((ROWS, 3 * B), F32),
            jax.ShapeDtypeStruct((3 * B, 2 * B), F32),
            jax.ShapeDtypeStruct((3 * B, 2 * B), F32),
        ),
        in_specs=[pl.BlockSpec((3 * B, ROWS // 2), lambda i: (0, i)), pl.BlockSpec((B, 3 * B), lambda i: (0, 0)), whole, whole],
        out_specs=(pl.BlockSpec((ROWS // 2, 3 * B), lambda i: (i, 0)), whole, whole),
        name="finish",
    )(wide_p, mixed, square_h, square_f)


def solution(mesh):
    return jax.shard_map(
        local,
        mesh=mesh,
        in_specs=(P("row", "col"), P()),
        out_specs=(P("row", None), P(), P()),
        check_vma=False,
    )
```
